32 devices in a mesh: dp: 8 (over z, x), seq: 4 (over y, core).
Axes of the slice: x: 2, y: 2, z: 4, core: 2. Of those that a mesh axis runs over, the one named last changes fastest.
Arguments:
- x_long: bfloat16 [32, 640, 768], P('dp', 'seq'), may hold values from -6 to 6
- x_short: bfloat16 [64, 160, 768], P(('dp', 'seq')), may hold values from -6 to 6
- seg_long: int32 [32, 640], P('dp'), may hold values from 0 to 4, never falling along the last dimension, each value on 1 to 256 neighbouring positions
- seg_short: int32 [64, 160], P(('dp', 'seq')), may hold values from 0 to 2, never falling along the last dimension, each value on 1 to 80 neighbouring positions
- pred_long: int32 [32, 640], P('dp', 'seq'), may hold values from 0 to 23
- target_long: int32 [32, 640], P('dp', 'seq'), may hold values from 0 to 23
- pred_short: int32 [64, 160], P(('dp', 'seq')), may hold values from 0 to 23
- target_short: int32 [64, 160], P(('dp', 'seq')), may hold values from 0 to 23
- query_weight: bfloat16 [768, 768], replicated, may hold values from -0.21875 to 0.21875
- key_weight: bfloat16 [768, 768], replicated, may hold values from -0.21875 to 0.21875
- value_weight: bfloat16 [768, 768], replicated, may hold values from -0.21875 to 0.21875
- out_weight: bfloat16 [768, 768], replicated, may hold values from -1.75 to 1.75
- up_weight: bfloat16 [768, 3072], replicated, may hold values from -0.21875 to 0.21875
- down_weight: bfloat16 [3072, 768], replicated, may hold values from -0.109375 to 0.109375
- vectors: float32 [8, 768], replicated, may hold values from -2.5 to 2.5, as said below
- up_bias: float32 [3072], replicated, may hold values from -3 to 3
- grad_long: bfloat16 [32, 640, 768], P(('dp', 'seq')), may hold values from -6 to 6
- grad_short: bfloat16 [64, 160, 768], P(('dp', 'seq')), may hold values from -6 to 6
Outputs:
- out_long: float32 [32, 640, 768], P(('dp', 'seq'))
- out_short: float32 [64, 160, 768], P(('dp', 'seq'))
- back_long: float32 [32, 640, 768], P('dp', 'seq')
- back_short: float32 [64, 160, 768], P(('dp', 'seq'))
- query_grad: float32 [768, 768], replicated
- key_grad: float32 [768, 768], replicated
- value_grad: float32 [768, 768], replicated
- out_grad: float32 [768, 768], replicated
- up_grad: float32 [768, 3072], replicated
- down_grad: float32 [3072, 768], replicated
- vector_grad: float32 [8, 768], replicated
- bias_grad: float32 [3072], replicated
- residue_counts: int32 [3, 24], replicated
The draws below stay inside these ranges and needn't reach their ends.
Inputs may be any that keep to these rules, and one draw needn't show every extreme that they name: `seg_long`: segment 0 is padding at the start of a row; other numbers are packed chains. `seg_short`: segment 0 is padding at the start of a row; other numbers are packed chains. `vectors`: rows 4 and 6 are norm gains near one; the others are biases and shifts.
All inputs are finite; a program needn't handle non-finite values.
Results may differ from the reference program's by a relative error of at most 0.02.
Values may be sent and summed in bfloat16 or wider, within the bound.
A program may use at most 256 MiB of HBM per device.

```python
import math
import jax
import jax.numpy as jnp
import numpy as np
from jax import lax

D = 768
HEADS = 12
HEAD = 64
FF = 3072
VOCAB = 24
LEN_L = 640
LEN_S = 160
NL = 32
NS = 64


def draw_vectors(key, part):
    normal_draw = jnp.clip(jax.random.normal(key, (8, D), jnp.float32), -5.0, 5.0)
    row_index = jnp.arange(8)[:, None]
    gain_rows = (row_index == 4) | (row_index == 6)
    return jnp.where(gain_rows, 1.0 + 0.1 * normal_draw, 0.5 * normal_draw)


def touch_ends(result, rng, least, top_value):
    longest = result.shape.index(max(result.shape))
    spots = []
    for shift in (0, 1):
        where = [jax.random.randint(jax.random.fold_in(rng, axis), (), 0, length) for axis, length in enumerate(result.shape)]
        where[longest] = (where[longest] + shift) % result.shape[longest]
        spots.append(tuple(where))
    return result.at[spots[0]].set(least).at[spots[1]].set(top_value)


def block_levels(own_key, shape, split, low, high):
    def one(dim, blocks):
        heights = jax.random.uniform(jax.random.fold_in(jax.random.fold_in(own_key, 6), dim), (blocks,), jnp.float32, low / len(split), high / len(split))
        return jnp.repeat(jnp.exp(heights), shape[dim] // blocks).reshape((-1,) + (1,) * (len(shape) - dim - 1))

    factor_of = one(*split[0])
    for cut in split[1:]:
        factor_of = factor_of * one(*cut)
    return factor_of


def profile(amount, total, reach, skew):
    loads = [(1 << 20) // math.isqrt(rank ** skew) + 1 for rank in range(2, amount + 1)]
    surplus, given = total - reach - (amount - 1), [1] * (amount - 1)
    while surplus > 0:
        candidates = [i for i in range(amount - 1) if given[i] < reach]
        whole, left = sum([loads[i] for i in candidates]), surplus
        for i in candidates:
            more = min(reach - given[i], max(1, left * loads[i] // whole), surplus)
            given[i] = given[i] + more
            surplus = surplus - more
    return np.array([reach] + given)


def uneven(own_key, number_of, total, bound, slope):
    if number_of == 2:
        one = jax.random.randint(own_key, (), max(1, total - bound), min(bound, total - 1) + 1)
        return jnp.stack([one, total - one])
    tallies = jnp.asarray(profile(number_of, total, bound, slope), jnp.int32)
    pairs = (number_of - 1) // 2
    giver, taker = tallies[1:1 + 2 * pairs:2], tallies[2:2 + 2 * pairs:2]
    slack = jnp.minimum(giver - 1, bound - taker)
    shifted = jax.random.randint(jax.random.fold_in(own_key, 1), (pairs,), 0, 1 << 20) % (slack + 1)
    tallies = tallies.at[1:1 + 2 * pairs:2].set(giver - shifted).at[2:2 + 2 * pairs:2].set(taker + shifted)
    return tallies[jax.random.permutation(jax.random.fold_in(own_key, 2), number_of)]


def noise(stream_key, dims, spread, limit, cuts=(), kind=jnp.bfloat16):
    entries = jax.random.normal(stream_key, dims, jnp.float32) * spread
    if len(cuts) > 0:
        entries = block_levels(stream_key, dims, cuts, -0.22, 0.18) * entries
    return jnp.clip(entries, min=-limit, max=limit).astype(kind)


def setup_inputs(seed: int = 0) -> dict:
    splits = jax.random.split(jax.random.key(seed), 19)
    x_long = noise(splits[0], (NL, LEN_L, D), 1.0, 6.0, ((0, 8), (1, 4)))
    x_short = noise(splits[1], (NS, LEN_S, D), 1.0, 6.0, ((0, 32),))
    seg_long = jax.vmap(lambda own: jnp.searchsorted(jnp.cumsum(uneven(own, 5, LEN_L, LEN_L * 2 // 5, 1)), jnp.arange(LEN_L), side="right"))(jax.random.split(splits[2], NL)).reshape((NL, LEN_L)).astype(jnp.int32)
    seg_short = jax.vmap(lambda own: jnp.searchsorted(jnp.cumsum(uneven(own, 3, LEN_S, LEN_S // 2, 1)), jnp.arange(LEN_S), side="right"))(jax.random.split(splits[3], NS)).reshape((NS, LEN_S)).astype(jnp.int32)
    pred_long = touch_ends(jax.random.randint(splits[4], (NL, LEN_L), 0, VOCAB), jax.random.fold_in(splits[4], 1), 0, VOCAB - 1).astype(jnp.int32)
    target_long = touch_ends(jax.random.randint(splits[5], (NL, LEN_L), 0, VOCAB), jax.random.fold_in(splits[5], 1), 0, VOCAB - 1).astype(jnp.int32)
    pred_short = touch_ends(jax.random.randint(splits[6], (NS, LEN_S), 0, VOCAB), jax.random.fold_in(splits[6], 1), 0, VOCAB - 1).astype(jnp.int32)
    target_short = touch_ends(jax.random.randint(splits[7], (NS, LEN_S), 0, VOCAB), jax.random.fold_in(splits[7], 1), 0, VOCAB - 1).astype(jnp.int32)
    query_weight = noise(splits[8], (D, D), D ** -0.5, 0.21875)
    key_weight = noise(splits[9], (D, D), D ** -0.5, 0.21875)
    value_weight = noise(splits[10], (D, D), D ** -0.5, 0.21875)
    out_weight = noise(splits[11], (D, D), (D // 64) ** -0.5, 1.75)
    up_weight = noise(splits[12], (D, FF), D ** -0.5, 0.21875)
    down_weight = noise(splits[13], (FF, D), FF ** -0.5, 0.109375)
    vectors = draw_vectors(jax.random.fold_in(splits[18], 71), 0)
    up_bias = noise(splits[15], (FF,), 0.5, 3.0, (), jnp.float32)
    grad_long = noise(splits[16], (NL, LEN_L, D), 1.0, 6.0, ((0, 32),))
    grad_short = noise(splits[17], (NS, LEN_S, D), 1.0, 6.0, ((0, 32),))
    return {"x_long": x_long, "x_short": x_short, "seg_long": seg_long, "seg_short": seg_short, "pred_long": pred_long, "target_long": target_long, "pred_short": pred_short, "target_short": target_short, "query_weight": query_weight, "key_weight": key_weight, "value_weight": value_weight, "out_weight": out_weight, "up_weight": up_weight, "down_weight": down_weight, "vectors": vectors, "up_bias": up_bias, "grad_long": grad_long, "grad_short": grad_short}


@jax.custom_vjp
def low(v):
    return lax.optimization_barrier(v.astype(jnp.bfloat16)).astype(jnp.float32)

@jax.custom_vjp
def low_back(v):
    return v

def low_keep(v):
    return (low(v), None)

def low_pass(kept, grad):
    return (grad,)

def back_keep(v):
    return (v, None)

def back_low(kept, grad):
    return (low(grad),)
low.defvjp(low_keep, low_pass)
low_back.defvjp(back_keep, back_low)

def matmul(matrix, weight):
    return jnp.dot(matrix, weight, precision=lax.Precision.HIGHEST)

def layer_norm(residual, gain_row, shift_row):
    centered = residual - lax.optimization_barrier(jnp.mean(residual, -1, keepdims=True))
    factor = lax.rsqrt(lax.optimization_barrier(jnp.mean(centered * centered, -1, keepdims=True)) + 1e-05)
    return centered * factor * gain_row + shift_row

def layer(parameters, single_row, segment):
    query_w, key_w, value_w, out_w, up_w, down_w, vectors, up_bias = parameters
    length = single_row.shape[0]
    queries = low_back(low(matmul(single_row, query_w) + vectors[0])).reshape(length, HEADS, HEAD)
    key_rows = low_back(low(matmul(single_row, key_w))).reshape(length, HEADS, HEAD)
    values = low_back(low(matmul(single_row, value_w) + vectors[1])).reshape(length, HEADS, HEAD)
    scores = jnp.einsum('qhe,khe->hqk', queries, key_rows, precision=lax.Precision.HIGHEST)
    scores = low_back(scores * HEAD ** (-0.5))
    allowed = (segment[:, None] == segment[None, :])[None]
    scores = jnp.where(allowed, scores, -1e+30)
    weights = jax.nn.softmax(scores, axis=-1)
    mixture = jnp.einsum('hqk,khe->qhe', weights, values, precision=lax.Precision.HIGHEST).reshape(length, D)
    mixture = low_back(low(mixture))
    branch = low_back(matmul(mixture, out_w) + vectors[2])
    hidden = layer_norm(single_row + branch, vectors[4], vectors[5])
    pre_act = low_back(matmul(low(hidden), up_w) + up_bias)
    activated = low(jax.nn.gelu(pre_act, approximate=False))
    second = hidden + low_back(matmul(activated, down_w) + vectors[3])
    return layer_norm(second, vectors[6], vectors[7])

def tally(predicted, target, segment):
    residues = jnp.arange(VOCAB, dtype=jnp.int32)[None, :]
    live_mask = (segment > 0).reshape(-1, 1)
    predicted = predicted.reshape(-1, 1)
    target = target.reshape(-1, 1)
    predicted_hot = (predicted == residues) & live_mask
    target_hot = (target == residues) & live_mask
    hit_hot = target_hot & (predicted == target)
    return jnp.stack([lax.optimization_barrier(jnp.sum(predicted_hot.astype(jnp.int32), 0)), lax.optimization_barrier(jnp.sum(target_hot.astype(jnp.int32), 0)), lax.optimization_barrier(jnp.sum(hit_hot.astype(jnp.int32), 0))])

def reference(x_long, x_short, seg_long, seg_short, pred_long, target_long, pred_short, target_short, query_weight, key_weight, value_weight, out_weight, up_weight, down_weight, vectors, up_bias, grad_long, grad_short):
    parameters = (query_weight.astype(jnp.float32), key_weight.astype(jnp.float32), value_weight.astype(jnp.float32), out_weight.astype(jnp.float32), up_weight.astype(jnp.float32), down_weight.astype(jnp.float32), vectors, up_bias)
    layer_step = jax.checkpoint(layer)

    def forward(params_in, long_rows, short_rows):

        def apply_long(entry_pair):
            return layer_step(params_in, entry_pair[0], entry_pair[1])
        long_out = lax.map(apply_long, (long_rows, seg_long))
        short_out = lax.map(apply_long, (short_rows, seg_short))
        return (long_out, short_out)
    outputs, pullback = jax.vjp(forward, parameters, x_long.astype(jnp.float32), x_short.astype(jnp.float32))
    gradients, back_long, back_short = pullback((grad_long.astype(jnp.float32), grad_short.astype(jnp.float32)))
    counts = tally(pred_long, target_long, seg_long) + tally(pred_short, target_short, seg_short)
    return (outputs[0], outputs[1], back_long, back_short, gradients[0], gradients[1], gradients[2], gradients[3], gradients[4], gradients[5], gradients[6], gradients[7], counts)
```

```python
import functools

import jax
import jax.numpy as jnp
from jax import lax
from jax.experimental import pallas as pl
from jax.experimental.pallas import tpu as pltpu
from jax.sharding import PartitionSpec as P

HEADS = 12
VOCAB = 24
LONG_REACH = 256

epsilon = 1e-05
blocked = -1e30


def project(matrix, weight):
    return jnp.dot(matrix, weight, preferred_element_type=jnp.float32)


def outer_sum(first_op, second_op):
    return lax.dot_general(
        first_op, second_op, (((0,), (0,)), ((), ())), preferred_element_type=jnp.float32
    )


def against(matrix, weight):
    return lax.dot_general(
        matrix, weight, (((1,), (1,)), ((), ())), preferred_element_type=jnp.float32
    )


def normalize(residual, gain_row, shift_row):
    centered = residual - jnp.mean(residual, -1, keepdims=True)
    factor = lax.rsqrt(jnp.mean(centered * centered, -1, keepdims=True) + epsilon)
    normed = centered * factor
    return (normed * gain_row + shift_row, normed, factor)


def normalize_back(upward, normed, factor, gain_row):
    scaled = upward * gain_row
    result = factor * (
        scaled
        - jnp.mean(scaled, -1, keepdims=True)
        - normed * jnp.mean(scaled * normed, -1, keepdims=True)
    )
    return (result, jnp.sum(upward * normed, 0), jnp.sum(upward, 0))


def blocks_of(long_len, short_len, short_rows):
    step = 128
    found = []
    for start in range(0, long_len, step):
        low = max(0, (start - LONG_REACH + 1) // step * step)
        high = min(long_len, -(-(start + step + LONG_REACH - 1) // step) * step)
        found.append((start, step, low, high, 0, 0))
    for row in range(short_rows):
        base = long_len + row * short_len
        found.append((base, short_len, base, base + short_len, base, row + 1))
    return found


def fill_bias(col_ref, row_ref, long_bias, short_bias, long_len, short_len, short_rows):
    col = col_ref[0:long_len, :]
    row = row_ref[0:1, 0:long_len]
    long_bias[...] = jnp.where(col == row, 0.0, blocked)
    for index in range(short_rows):
        base = long_len + index * short_len
        col = col_ref[base : base + short_len, :]
        row = row_ref[1 + index : 2 + index, 0:short_len]
        short_bias[index] = jnp.where(col == row, 0.0, blocked)


def bias_at(long_bias, short_bias, first, first_count, low, high, base, index):
    if index == 0:
        return long_bias[first : first + first_count, low:high]
    return short_bias[index - 1]


def two_heads(block, lanes, scale):
    half = block.shape[1] // 2
    zero = jnp.zeros_like(block)
    if scale != 1.0:
        block = block * scale
    return jnp.concatenate(
        [jnp.where(lanes < half, block, zero), jnp.where(lanes < half, zero, block)], 0
    )


def attend_kernel(sizes, scale, q_ref, k_ref, v_ref, col_ref, row_ref, o_ref, long_bias, short_bias):
    @pl.when(pl.program_id(0) == 0)
    def _():
        fill_bias(col_ref, row_ref, long_bias, short_bias, *sizes)

    for first, count, low, high, base, index in blocks_of(*sizes):
        lanes = lax.broadcasted_iota(jnp.int32, (count, 128), 1)
        pair = two_heads(q_ref[first : first + count, :], lanes, scale)
        scores = against(pair, k_ref[low:high, :])
        bias = bias_at(long_bias, short_bias, first, count, low, high, base, index)
        scores = scores + jnp.concatenate([bias, bias], 0)
        highest = jnp.max(scores, -1, keepdims=True)
        weights = jnp.exp(scores - highest)
        summed = jnp.sum(weights, -1, keepdims=True)
        mixed = project(weights.astype(jnp.bfloat16), v_ref[low:high, :]) / summed
        o_ref[first : first + count, :] = jnp.where(
            lanes < 64, mixed[:count], mixed[count:]
        ).astype(jnp.bfloat16)


def attend_back_kernel(
    sizes,
    scale,
    q_ref,
    k_ref,
    v_ref,
    g_ref,
    col_ref,
    row_ref,
    dq_ref,
    dk_ref,
    dv_ref,
    long_bias,
    short_bias,
    k_sum,
    v_sum,
):
    @pl.when(pl.program_id(0) == 0)
    def _():
        fill_bias(col_ref, row_ref, long_bias, short_bias, *sizes)

    k_sum[...] = jnp.zeros_like(k_sum)
    v_sum[...] = jnp.zeros_like(v_sum)
    for first, count, low, high, base, index in blocks_of(*sizes):
        lanes = lax.broadcasted_iota(jnp.int32, (count, 128), 1)
        pair = two_heads(q_ref[first : first + count, :], lanes, scale)
        upward = two_heads(g_ref[first : first + count, :], lanes, 1.0)
        keys = k_ref[low:high, :]
        scores = against(keys, pair)
        if index == 0:
            bias = long_bias[low:high, first : first + count]
        else:
            bias = short_bias[index - 1]
        scores = scores + jnp.concatenate([bias, bias], 1)
        highest = jnp.max(scores, 0, keepdims=True)
        weights = jnp.exp(scores - highest)
        weights = weights * (1.0 / jnp.sum(weights, 0, keepdims=True))
        weight_grad = against(v_ref[low:high, :], upward)
        delta = jnp.sum(weights * weight_grad, 0, keepdims=True)
        score_grad = (weights * (weight_grad - delta)).astype(jnp.bfloat16)
        v_sum[low:high, :] += project(weights.astype(jnp.bfloat16), upward)
        k_sum[low:high, :] += project(score_grad, pair)
        q_part = outer_sum(score_grad, keys) * scale
        dq_ref[first : first + count, :] = jnp.where(lanes < 64, q_part[:count], q_part[count:]).astype(
            jnp.bfloat16
        )
    dk_ref[...] = k_sum[...].astype(jnp.bfloat16)
    dv_ref[...] = v_sum[...].astype(jnp.bfloat16)


def attention_calls(sizes, rows, width, scale):
    long_len, short_len, short_rows = sizes
    pairs = width // 128
    column = pl.BlockSpec((rows, 128), lambda i: (0, i))
    col_spec = pl.BlockSpec((rows, 1), lambda i: (0, 0))
    row_spec = pl.BlockSpec((1 + short_rows, long_len), lambda i: (0, 0))
    shape = jax.ShapeDtypeStruct((rows, width), jnp.bfloat16)
    bias = [
        pltpu.VMEM((long_len, long_len), jnp.float32),
        pltpu.VMEM((short_rows, short_len, short_len), jnp.float32),
    ]
    forward = pl.pallas_call(
        functools.partial(attend_kernel, sizes, scale),
        grid=(pairs,),
        in_specs=[column] * 3 + [col_spec, row_spec],
        out_specs=column,
        out_shape=shape,
        scratch_shapes=bias,
        name="attend",
    )
    backward = pl.pallas_call(
        functools.partial(attend_back_kernel, sizes, scale),
        grid=(pairs,),
        in_specs=[column] * 4 + [col_spec, row_spec],
        out_specs=[column] * 3,
        out_shape=[shape] * 3,
        scratch_shapes=bias + [pltpu.VMEM((rows, 128), jnp.float32)] * 2,
        name="attend_back",
    )
    return forward, backward


def tally(predicted, target, segment):
    residues = jnp.arange(VOCAB, dtype=jnp.int32)[None, :]
    live_mask = (segment > 0).reshape(-1, 1)
    predicted = predicted.reshape(-1, 1)
    target = target.reshape(-1, 1)
    predicted_hot = (predicted == residues) & live_mask
    target_hot = (target == residues) & live_mask
    hit_hot = target_hot & (predicted == target)
    return jnp.stack(
        [
            jnp.sum(predicted_hot.astype(jnp.float32), 0),
            jnp.sum(target_hot.astype(jnp.float32), 0),
            jnp.sum(hit_hot.astype(jnp.float32), 0),
        ]
    )


def local(
    x_long,
    x_short,
    seg_long,
    seg_short,
    pred_long,
    target_long,
    pred_short,
    target_short,
    query_weight,
    key_weight,
    value_weight,
    out_weight,
    up_weight,
    down_weight,
    vectors,
    up_bias,
    grad_long,
    grad_short,
):
    local_len, width = x_long.shape[1:]
    short_rows, short_len = x_short.shape[:2]
    groups = lax.axis_size("seq")
    position = lax.axis_index("seq")
    row_len = local_len * groups
    rows_here = x_long.shape[0] // groups
    split = rows_here * row_len
    total = split + short_rows * short_len
    sizes = (row_len, short_len, short_rows)
    forward, backward = attention_calls(sizes, total, width, (width // HEADS) ** (-0.5))

    seg_row = lax.dynamic_slice_in_dim(seg_long, position * rows_here, rows_here, 0)
    seg_local = lax.dynamic_slice_in_dim(seg_long, position * local_len, local_len, 1)
    seg_rows = jnp.concatenate(
        [seg_row, jnp.pad(seg_short, ((0, 0), (0, row_len - short_len)), constant_values=-1)], 0
    )
    seg_column = jnp.concatenate([seg_row.reshape(-1, 1), seg_short.reshape(-1, 1)], 0)

    moved = lax.all_to_all(x_long, "seq", split_axis=0, concat_axis=1, tiled=True)
    tokens = jnp.concatenate([moved.reshape(split, width), x_short.reshape(-1, width)], 0)
    queries = (project(tokens, query_weight) + vectors[0]).astype(jnp.bfloat16)
    key_rows = project(tokens, key_weight).astype(jnp.bfloat16)
    value_rows = (project(tokens, value_weight) + vectors[1]).astype(jnp.bfloat16)
    mixture = forward(queries, key_rows, value_rows, seg_column, seg_rows)
    branch = project(mixture, out_weight) + vectors[2]
    hidden, normed_one, factor_one = normalize(
        tokens.astype(jnp.float32) + branch, vectors[4], vectors[5]
    )
    hidden_low = hidden.astype(jnp.bfloat16)
    pre_act = project(hidden_low, up_weight) + up_bias
    activated, gelu_back = jax.vjp(lambda inner: jax.nn.gelu(inner, approximate=False), pre_act)
    act_low = activated.astype(jnp.bfloat16)
    output, normed_two, factor_two = normalize(
        hidden + project(act_low, down_weight) + vectors[3], vectors[6], vectors[7]
    )
    out_long = output[:split].reshape(rows_here, row_len, width)
    out_short = output[split:].reshape(short_rows, short_len, width)
    upstream = jnp.concatenate(
        [grad_long.reshape(split, width), grad_short.reshape(-1, width)], 0
    ).astype(jnp.float32)
    second_grad, gain_two, shift_two = normalize_back(upstream, normed_two, factor_two, vectors[6])
    down_in = second_grad.astype(jnp.bfloat16)
    down_grad = outer_sum(act_low, down_in)
    down_total = jnp.sum(down_in.astype(jnp.float32), 0)
    pre_grad = gelu_back(against(down_in, down_weight))[0].astype(jnp.bfloat16)
    up_grad = outer_sum(hidden_low, pre_grad)
    bias_total = jnp.sum(pre_grad.astype(jnp.float32), 0)
    hidden_grad = second_grad + against(pre_grad, up_weight)
    first_grad, gain_one, shift_one = normalize_back(
        hidden_grad, normed_one, factor_one, vectors[4]
    )
    branch_in = first_grad.astype(jnp.bfloat16)
    out_grad = outer_sum(mixture, branch_in)
    out_total = jnp.sum(branch_in.astype(jnp.float32), 0)
    mixture_grad = against(branch_in, out_weight).astype(jnp.bfloat16)
    query_in, key_in, value_in = backward(
        queries, key_rows, value_rows, mixture_grad, seg_column, seg_rows
    )
    query_grad = outer_sum(tokens, query_in)
    key_grad = outer_sum(tokens, key_in)
    value_grad = outer_sum(tokens, value_in)
    token_grad = (
        first_grad
        + against(query_in, query_weight)
        + against(key_in, key_weight)
        + against(value_in, value_weight)
    )
    returned = lax.all_to_all(
        token_grad[:split].reshape(rows_here, row_len, width).astype(jnp.bfloat16),
        "seq",
        split_axis=1,
        concat_axis=0,
        tiled=True,
    )
    back_long = returned.astype(jnp.float32)
    back_short = token_grad[split:].reshape(short_rows, short_len, width)
    counts = tally(pred_long, target_long, seg_local) + tally(pred_short, target_short, seg_short)
    small = jnp.concatenate(
        [
            jnp.stack(
                [
                    jnp.sum(query_in.astype(jnp.float32), 0),
                    jnp.sum(value_in.astype(jnp.float32), 0),
                    out_total,
                    down_total,
                    gain_one,
                    shift_one,
                    gain_two,
                    shift_two,
                ]
            ),
            bias_total.reshape(-1, width),
            jnp.pad(counts.reshape(1, -1), ((0, 0), (0, width - counts.size))),
        ],
        0,
    )
    members = tuple(
        part.astype(jnp.bfloat16)
        for part in (query_grad, key_grad, value_grad, out_grad, up_grad, down_grad)
    )
    summed = lax.psum(members, ("dp", "seq"))
    small = lax.psum(small, ("dp", "seq"))
    return (
        out_long,
        out_short,
        back_long,
        back_short,
        *(part.astype(jnp.float32) for part in summed),
        small[:8],
        small[8:-1].reshape(-1),
        small[-1, : counts.size].reshape(counts.shape).astype(jnp.int32),
    )


def solution(mesh):
    placed = (
        P("dp", "seq", None),
        P(("dp", "seq"), None, None),
        P("dp", None),
        P(("dp", "seq"), None),
        P("dp", "seq"),
        P("dp", "seq"),
        P(("dp", "seq"), None),
        P(("dp", "seq"), None),
        P(),
        P(),
        P(),
        P(),
        P(),
        P(),
        P(),
        P(),
        P(("dp", "seq"), None, None),
        P(("dp", "seq"), None, None),
    )
    return jax.shard_map(
        local,
        mesh=mesh,
        in_specs=placed,
        out_specs=(
            P(("dp", "seq"), None, None),
            P(("dp", "seq"), None, None),
            P("dp", "seq", None),
            P(("dp", "seq"), None, None),
            P(),
            P(),
            P(),
            P(),
            P(),
            P(),
            P(),
            P(),
            P(),
        ),
        check_vma=False,
    )
```

```python
import functools

import jax
import jax.numpy as jnp
from jax import lax
from jax.experimental import pallas as pl
from jax.experimental.pallas import tpu as pltpu
from jax.sharding import PartitionSpec as P

HEADS = 12
VOCAB = 24
LONG_REACH = 256

epsilon = 1e-05
blocked = -1e30


def project(matrix, weight):
    return jnp.dot(matrix, weight, preferred_element_type=jnp.float32)


def outer_sum(first_op, second_op):
    return lax.dot_general(
        first_op, second_op, (((0,), (0,)), ((), ())), preferred_element_type=jnp.float32
    )


def against(matrix, weight):
    return lax.dot_general(
        matrix, weight, (((1,), (1,)), ((), ())), preferred_element_type=jnp.float32
    )


def normalize(residual, gain_row, shift_row):
    centered = residual - jnp.mean(residual, -1, keepdims=True)
    factor = lax.rsqrt(jnp.mean(centered * centered, -1, keepdims=True) + epsilon)
    normed = centered * factor
    return (normed * gain_row + shift_row, normed, factor)


def normalize_back(upward, normed, factor, gain_row):
    scaled = upward * gain_row
    result = factor * (
        scaled
        - jnp.mean(scaled, -1, keepdims=True)
        - normed * jnp.mean(scaled * normed, -1, keepdims=True)
    )
    return (result, jnp.sum(upward * normed, 0), jnp.sum(upward, 0))


def blocks_of(long_len, short_len, short_rows):
    step = 128
    found = []
    for start in range(0, long_len, step):
        low = max(0, (start - LONG_REACH + 1) // step * step)
        high = min(long_len, -(-(start + step + LONG_REACH - 1) // step) * step)
        found.append((start, step, low, high, 0, 0))
    for row in range(short_rows):
        base = long_len + row * short_len
        found.append((base, short_len, base, base + short_len, base, row + 1))
    return found


def fill_bias(col_ref, row_ref, long_bias, short_bias, long_len, short_len, short_rows):
    col = col_ref[0:long_len, :]
    row = row_ref[0:1, 0:long_len]
    long_bias[...] = jnp.where(col == row, 0.0, blocked)
    for index in range(short_rows):
        base = long_len + index * short_len
        col = col_ref[base : base + short_len, :]
        row = row_ref[1 + index : 2 + index, 0:short_len]
        short_bias[index] = jnp.where(col == row, 0.0, blocked)


def bias_at(long_bias, short_bias, first, first_count, low, high, base, index):
    if index == 0:
        return long_bias[first : first + first_count, low:high]
    return short_bias[index - 1]


def two_heads(block, lanes, scale):
    half = block.shape[1] // 2
    zero = jnp.zeros_like(block)
    if scale != 1.0:
        block = block * scale
    return jnp.concatenate(
        [jnp.where(lanes < half, block, zero), jnp.where(lanes < half, zero, block)], 0
    )


def attend_kernel(sizes, scale, q_ref, k_ref, v_ref, col_ref, row_ref, o_ref, long_bias, short_bias):
    @pl.when(pl.program_id(0) == 0)
    def _():
        fill_bias(col_ref, row_ref, long_bias, short_bias, *sizes)

    for first, count, low, high, base, index in blocks_of(*sizes):
        lanes = lax.broadcasted_iota(jnp.int32, (count, 128), 1)
        pair = two_heads(q_ref[first : first + count, :], lanes, scale)
        scores = against(pair, k_ref[low:high, :])
        bias = bias_at(long_bias, short_bias, first, count, low, high, base, index)
        scores = scores + jnp.concatenate([bias, bias], 0)
        highest = jnp.max(scores, -1, keepdims=True)
        weights = jnp.exp(scores - highest)
        summed = jnp.sum(weights, -1, keepdims=True)
        mixed = project(weights.astype(jnp.bfloat16), v_ref[low:high, :]) / summed
        o_ref[first : first + count, :] = jnp.where(
            lanes < 64, mixed[:count], mixed[count:]
        ).astype(jnp.bfloat16)


def attend_back_kernel(
    sizes,
    scale,
    q_ref,
    k_ref,
    v_ref,
    g_ref,
    col_ref,
    row_ref,
    dq_ref,
    dk_ref,
    dv_ref,
    long_bias,
    short_bias,
    k_sum,
    v_sum,
):
    @pl.when(pl.program_id(0) == 0)
    def _():
        fill_bias(col_ref, row_ref, long_bias, short_bias, *sizes)

    k_sum[...] = jnp.zeros_like(k_sum)
    v_sum[...] = jnp.zeros_like(v_sum)
    for first, count, low, high, base, index in blocks_of(*sizes):
        lanes = lax.broadcasted_iota(jnp.int32, (count, 128), 1)
        pair = two_heads(q_ref[first : first + count, :], lanes, scale)
        upward = two_heads(g_ref[first : first + count, :], lanes, 1.0)
        keys = k_ref[low:high, :]
        scores = against(keys, pair)
        if index == 0:
            bias = long_bias[low:high, first : first + count]
        else:
            bias = short_bias[index - 1]
        scores = scores + jnp.concatenate([bias, bias], 1)
        highest = jnp.max(scores, 0, keepdims=True)
        weights = jnp.exp(scores - highest)
        weights = weights * (1.0 / jnp.sum(weights, 0, keepdims=True))
        weight_grad = against(v_ref[low:high, :], upward)
        delta = jnp.sum(weights * weight_grad, 0, keepdims=True)
        score_grad = (weights * (weight_grad - delta)).astype(jnp.bfloat16)
        v_sum[low:high, :] += project(weights.astype(jnp.bfloat16), upward)
        k_sum[low:high, :] += project(score_grad, pair)
        q_part = outer_sum(score_grad, keys) * scale
        dq_ref[first : first + count, :] = jnp.where(lanes < 64, q_part[:count], q_part[count:]).astype(
            jnp.bfloat16
        )
    dk_ref[...] = k_sum[...].astype(jnp.bfloat16)
    dv_ref[...] = v_sum[...].astype(jnp.bfloat16)


def attention_calls(sizes, rows, width, scale):
    long_len, short_len, short_rows = sizes
    pairs = width // 128
    column = pl.BlockSpec((rows, 128), lambda i: (0, i))
    col_spec = pl.BlockSpec((rows, 1), lambda i: (0, 0))
    row_spec = pl.BlockSpec((1 + short_rows, long_len), lambda i: (0, 0))
    shape = jax.ShapeDtypeStruct((rows, width), jnp.bfloat16)
    bias = [
        pltpu.VMEM((long_len, long_len), jnp.float32),
        pltpu.VMEM((short_rows, short_len, short_len), jnp.float32),
    ]
    forward = pl.pallas_call(
        functools.partial(attend_kernel, sizes, scale),
        grid=(pairs,),
        in_specs=[column] * 3 + [col_spec, row_spec],
        out_specs=column,
        out_shape=shape,
        scratch_shapes=bias,
        name="attend",
    )
    backward = pl.pallas_call(
        functools.partial(attend_back_kernel, sizes, scale),
        grid=(pairs,),
        in_specs=[column] * 4 + [col_spec, row_spec],
        out_specs=[column] * 3,
        out_shape=[shape] * 3,
        scratch_shapes=bias + [pltpu.VMEM((rows, 128), jnp.float32)] * 2,
        name="attend_back",
    )
    return forward, backward


def physical_axes(mesh):
    first = mesh.devices[0, 0]
    found = {}
    for place, name in enumerate(("x", "y", "z", "core")):

        def at(device):
            return device.core_on_chip if name == "core" else device.coords[place]

        for axis, line in (("dp", mesh.devices[:, 0]), ("seq", mesh.devices[0, :])):
            values = [at(device) - at(first) for device in line]
            size = max(values) + 1
            if size > 1:
                stride = values.index(1)
                assert values == [i // stride % size for i in range(len(values))]
                found[name] = (axis, stride, size)
    return found


def reduce_kernel(axes, orders, chunks, up_ref, down_ref, square_ref, small_ref, full, small_out, buf, *scratch):
    colors, rows, width = buf.shape
    depth = len(orders[0])
    lands = scratch[:depth]
    small_land, load_sem, send_sem, recv_sem, small_send, small_recv = scratch[depth:]
    chunk = rows // chunks
    spots = {
        name: lax.rem(lax.axis_index(axis) // stride, size)
        for name, (axis, stride, size) in axes.items()
    }

    def peer(name, change):
        axis, stride, size = axes[name]
        target = {other: lax.axis_index(other) for other in ("dp", "seq")}
        target[axis] = target[axis] + change * stride
        return (target["dp"], target["seq"])

    loads = []
    for block in range(up_ref.shape[1] // width):
        loads.append((up_ref.at[:, block * width : (block + 1) * width], buf.at[0, block * width : (block + 1) * width]))
    loads.append((down_ref, buf.at[1]))
    loads.append((square_ref, buf.at[2]))
    copies = [
        pltpu.make_async_copy(source, target, load_sem.at[i]) for i, (source, target) in enumerate(loads)
    ]
    for copy in copies:
        copy.start()

    barrier = pltpu.get_barrier_semaphore()
    greeted = 0
    for name, (axis, stride, size) in axes.items():
        for step in range(1, size):
            change = lax.rem(spots[name] + step, size) - spots[name]
            pl.semaphore_signal(
                barrier, inc=1, device_id=peer(name, change), device_id_type=pl.DeviceIdType.MESH
            )
            greeted += 1
    pl.semaphore_wait(barrier, greeted)
    for copy in copies:
        copy.wait()

    def message(color, level, phase, way, k, name, source, target, change):
        return pltpu.make_async_remote_copy(
            src_ref=source,
            dst_ref=target,
            send_sem=send_sem.at[color, level, phase, way, k],
            recv_sem=recv_sem.at[color, level, phase, way, k],
            device_id=peer(name, change),
            device_id_type=pl.DeviceIdType.MESH,
        )

    def plan(color, level, k):
        size = chunk >> (level + 1)
        start = k * chunk
        active = None
        for other in range(level):
            name = orders[color][other]
            last = axes[name][2] - 1
            start = start + jnp.where(spots[name] == last, chunk >> (other + 1), 0)
            if last > 1:
                ends = (spots[name] == 0) | (spots[name] == last)
                active = ends if active is None else active & ends
        return size, start, active

    def guarded(condition, active, body):
        pl.when(condition if active is None else condition & active)(body)

    def reduce_slot(color, level, slot, k):
        name = orders[color][level]
        last = axes[name][2] - 1
        size, start, active = plan(color, level, k)
        for way in range(2):
            place = slot if way == 1 else last - slot
            held = buf.at[color, pl.ds(pl.multiple_of(start + way * size, 16), size)]
            spot = k if lands[level].shape[1] < 2 * chunks * size else 2 * k + way
            land = lands[level].at[color, pl.ds(pl.multiple_of(spot * size, 16), size)]
            change = 1 if way == 1 else -1
            copy = message(color, level, 0, way, k, name, held, land, change)

            into = held
            if level == depth - 1 and slot == last:
                into = full.at[color, pl.ds(pl.multiple_of(start + way * size, 16), size)]

            def body(copy=copy, held=held, land=land, into=into):
                if slot > 0:
                    copy.wait_recv()
                    into[...] = (held[...].astype(jnp.float32) + land[...].astype(jnp.float32)).astype(
                        jnp.bfloat16
                    )
                if slot < last:
                    copy.start()

            guarded(spots[name] == place, active, body)

    def spread_slot(color, level, slot, k):
        name = orders[color][level]
        last = axes[name][2] - 1
        size, start, active = plan(color, level, k)
        for way in range(2):
            place = last - slot if way == 1 else slot
            held = full.at[color, pl.ds(pl.multiple_of(start + way * size, 16), size)]
            change = -1 if way == 1 else 1
            copy = message(color, level, 1, way, k, name, held, held, change)

            def body(copy=copy):
                if slot > 0:
                    copy.wait_recv()
                if slot < last:
                    copy.start()

            guarded(spots[name] == place, active, body)

    def sent(color, level, k):
        name = orders[color][level]
        last = axes[name][2] - 1
        size, start, active = plan(color, level, k)
        for way in range(2):
            held = buf.at[color, pl.ds(pl.multiple_of(start + way * size, 16), size)]
            for phase in range(2):
                copy = message(color, level, phase, way, k, name, held, held, 1)
                stays = spots[name] == (last if (way == 1) == (phase == 0) else 0)
                guarded(jnp.logical_not(stays), active, copy.wait_send)

    small_order = tuple(axes)

    def small_copy(level, step):
        name = small_order[level]
        size = axes[name][2]
        change = lax.rem(spots[name] + step, size) - spots[name]
        slot = sum(axes[other][2] for other in small_order[:level])
        return pltpu.make_async_remote_copy(
            src_ref=small_out,
            dst_ref=small_land.at[slot + step],
            send_sem=small_send.at[slot + step],
            recv_sem=small_recv.at[slot + step],
            device_id=peer(name, change),
            device_id_type=pl.DeviceIdType.MESH,
        )

    def small_start(level):
        for step in range(1, axes[small_order[level]][2]):
            small_copy(level, step).start()

    def small_finish(level):
        name = small_order[level]
        size = axes[name][2]
        slot = sum(axes[other][2] for other in small_order[:level])
        for step in range(1, size):
            small_copy(level, step).wait()
        small_land[slot] = small_out[...]
        total = None
        for place in range(size):
            term = small_land[slot + lax.rem(spots[name] - place + size, size)]
            total = term if total is None else total + term
        small_out[...] = total

    small_out[...] = small_ref[...]
    hops = sum(size - 1 for _, _, size in axes.values())

    def tick(t, carry):
        for color in range(colors):
            base = 0
            for level in range(depth):
                last = axes[orders[color][level]][2] - 1
                for slot in range(last + 1):
                    k = t - (base + slot)

                    @pl.when((k >= 0) & (k < chunks))
                    def _(color=color, level=level, slot=slot, k=k):
                        reduce_slot(color, level, slot, k)

                base += last
            for level in reversed(range(depth)):
                last = axes[orders[color][level]][2] - 1
                for slot in range(last + 1):
                    k = t - (base + slot)

                    @pl.when((k >= 0) & (k < chunks))
                    def _(color=color, level=level, slot=slot, k=k):
                        spread_slot(color, level, slot, k)

                base += last
        for level in range(depth):

            @pl.when(t == 2 * level)
            def _(level=level):
                small_start(level)

            @pl.when(t == 2 * level + 1)
            def _(level=level):
                small_finish(level)

        return carry

    lax.fori_loop(0, chunks + 2 * hops, tick, 0)

    def drain(k, carry):
        for color in range(colors):
            for level in range(depth):
                sent(color, level, k)
        return carry

    lax.fori_loop(0, chunks, drain, 0)


def reduce_call(axes, up, down, square, small):
    rows, width = down.shape
    colors, chunks = 3, 6
    turn = [name for name in ("x", "y", "z") if name in axes]
    first = [name for name in ("core",) if name in axes]
    orders = [first + turn[i:] + turn[:i] for i in range(3)]
    depth = len(orders[0])
    steps = sum(size for _, _, size in axes.values())
    count = up.shape[1] // width + 2
    sems = (colors, depth, 2, 2, chunks)
    lands = [
        rows >> (level + all(axes[order[level]][2] == 2 for order in orders)) for level in range(depth)
    ]
    return pl.pallas_call(
        functools.partial(reduce_kernel, axes, orders, chunks),
        in_specs=[pl.BlockSpec(memory_space=pl.ANY)] * 3 + [pl.BlockSpec(memory_space=pltpu.VMEM)],
        out_specs=[pl.BlockSpec(memory_space=pltpu.VMEM)] * 2,
        out_shape=[
            jax.ShapeDtypeStruct((colors, rows, width), jnp.bfloat16),
            jax.ShapeDtypeStruct(small.shape, jnp.float32),
        ],
        scratch_shapes=[pltpu.VMEM((colors, rows, width), jnp.bfloat16)]
        + [pltpu.VMEM((colors, size, width), jnp.bfloat16) for size in lands]
        + [
            pltpu.VMEM((steps,) + small.shape, jnp.float32),
            pltpu.SemaphoreType.DMA((count,)),
            pltpu.SemaphoreType.DMA(sems),
            pltpu.SemaphoreType.DMA(sems),
            pltpu.SemaphoreType.DMA((steps,)),
            pltpu.SemaphoreType.DMA((steps,)),
        ],
        compiler_params=pltpu.CompilerParams(
            collective_id=0, has_side_effects=True, vmem_limit_bytes=60 * 1024 * 1024
        ),
        name="reduce",
    )(up, down, square, small)


def tally(predicted, target, segment):
    residues = jnp.arange(VOCAB, dtype=jnp.int32)[None, :]
    live_mask = (segment > 0).reshape(-1, 1)
    predicted = predicted.reshape(-1, 1)
    target = target.reshape(-1, 1)
    predicted_hot = (predicted == residues) & live_mask
    target_hot = (target == residues) & live_mask
    hit_hot = target_hot & (predicted == target)
    return jnp.stack(
        [
            jnp.sum(predicted_hot.astype(jnp.float32), 0),
            jnp.sum(target_hot.astype(jnp.float32), 0),
            jnp.sum(hit_hot.astype(jnp.float32), 0),
        ]
    )


def local(
    axes,
    x_long,
    x_short,
    seg_long,
    seg_short,
    pred_long,
    target_long,
    pred_short,
    target_short,
    query_weight,
    key_weight,
    value_weight,
    out_weight,
    up_weight,
    down_weight,
    vectors,
    up_bias,
    grad_long,
    grad_short,
):
    local_len, width = x_long.shape[1:]
    short_rows, short_len = x_short.shape[:2]
    groups = lax.axis_size("seq")
    position = lax.axis_index("seq")
    row_len = local_len * groups
    rows_here = x_long.shape[0] // groups
    split = rows_here * row_len
    total = split + short_rows * short_len
    sizes = (row_len, short_len, short_rows)
    forward, backward = attention_calls(sizes, total, width, (width // HEADS) ** (-0.5))

    seg_row = lax.dynamic_slice_in_dim(seg_long, position * rows_here, rows_here, 0)
    seg_local = lax.dynamic_slice_in_dim(seg_long, position * local_len, local_len, 1)
    seg_rows = jnp.concatenate(
        [seg_row, jnp.pad(seg_short, ((0, 0), (0, row_len - short_len)), constant_values=-1)], 0
    )
    seg_column = jnp.concatenate([seg_row.reshape(-1, 1), seg_short.reshape(-1, 1)], 0)

    moved = lax.all_to_all(x_long, "seq", split_axis=0, concat_axis=1, tiled=True)
    tokens = jnp.concatenate([moved.reshape(split, width), x_short.reshape(-1, width)], 0)
    queries = (project(tokens, query_weight) + vectors[0]).astype(jnp.bfloat16)
    key_rows = project(tokens, key_weight).astype(jnp.bfloat16)
    value_rows = (project(tokens, value_weight) + vectors[1]).astype(jnp.bfloat16)
    mixture = forward(queries, key_rows, value_rows, seg_column, seg_rows)
    branch = project(mixture, out_weight) + vectors[2]
    hidden, normed_one, factor_one = normalize(
        tokens.astype(jnp.float32) + branch, vectors[4], vectors[5]
    )
    hidden_low = hidden.astype(jnp.bfloat16)
    pre_act = project(hidden_low, up_weight) + up_bias
    activated, gelu_back = jax.vjp(lambda inner: jax.nn.gelu(inner, approximate=False), pre_act)
    act_low = activated.astype(jnp.bfloat16)
    output, normed_two, factor_two = normalize(
        hidden + project(act_low, down_weight) + vectors[3], vectors[6], vectors[7]
    )
    out_long = output[:split].reshape(rows_here, row_len, width)
    out_short = output[split:].reshape(short_rows, short_len, width)
    upstream = jnp.concatenate(
        [grad_long.reshape(split, width), grad_short.reshape(-1, width)], 0
    ).astype(jnp.float32)
    second_grad, gain_two, shift_two = normalize_back(upstream, normed_two, factor_two, vectors[6])
    down_in = second_grad.astype(jnp.bfloat16)
    down_grad = outer_sum(act_low, down_in)
    down_total = jnp.sum(down_in.astype(jnp.float32), 0)
    pre_grad = gelu_back(against(down_in, down_weight))[0].astype(jnp.bfloat16)
    up_grad = outer_sum(hidden_low, pre_grad)
    bias_total = jnp.sum(pre_grad.astype(jnp.float32), 0)
    hidden_grad = second_grad + against(pre_grad, up_weight)
    first_grad, gain_one, shift_one = normalize_back(
        hidden_grad, normed_one, factor_one, vectors[4]
    )
    branch_in = first_grad.astype(jnp.bfloat16)
    out_grad = outer_sum(mixture, branch_in)
    out_total = jnp.sum(branch_in.astype(jnp.float32), 0)
    mixture_grad = against(branch_in, out_weight).astype(jnp.bfloat16)
    query_in, key_in, value_in = backward(
        queries, key_rows, value_rows, mixture_grad, seg_column, seg_rows
    )
    query_grad = outer_sum(tokens, query_in)
    key_grad = outer_sum(tokens, key_in)
    value_grad = outer_sum(tokens, value_in)
    token_grad = (
        first_grad
        + against(query_in, query_weight)
        + against(key_in, key_weight)
        + against(value_in, value_weight)
    )
    returned = lax.all_to_all(
        token_grad[:split].reshape(rows_here, row_len, width).astype(jnp.bfloat16),
        "seq",
        split_axis=1,
        concat_axis=0,
        tiled=True,
    )
    back_long = returned.astype(jnp.float32)
    back_short = token_grad[split:].reshape(short_rows, short_len, width)
    counts = tally(pred_long, target_long, seg_local) + tally(pred_short, target_short, seg_short)
    small = jnp.concatenate(
        [
            jnp.stack(
                [
                    jnp.sum(query_in.astype(jnp.float32), 0),
                    jnp.sum(value_in.astype(jnp.float32), 0),
                    out_total,
                    down_total,
                    gain_one,
                    shift_one,
                    gain_two,
                    shift_two,
                ]
            ),
            bias_total.reshape(-1, width),
            jnp.pad(counts.reshape(1, -1), ((0, 3), (0, width - counts.size))),
        ],
        0,
    )
    square = jnp.concatenate([query_grad, key_grad, value_grad, out_grad], 0).astype(jnp.bfloat16)
    summed, small = reduce_call(
        axes, up_grad.astype(jnp.bfloat16), down_grad.astype(jnp.bfloat16), square, small
    )
    summed = summed.astype(jnp.float32)
    up_total = jnp.concatenate([summed[0, i : i + width] for i in range(0, up_grad.shape[1], width)], 1)
    vector_rows = 8 + up_bias.size // width
    return (
        out_long,
        out_short,
        back_long,
        back_short,
        *(summed[2, i * width : (i + 1) * width] for i in range(4)),
        up_total,
        summed[1],
        small[:8],
        small[8:vector_rows].reshape(-1),
        small[vector_rows, : counts.size].reshape(counts.shape).astype(jnp.int32),
    )


def solution(mesh):
    placed = (
        P("dp", "seq", None),
        P(("dp", "seq"), None, None),
        P("dp", None),
        P(("dp", "seq"), None),
        P("dp", "seq"),
        P("dp", "seq"),
        P(("dp", "seq"), None),
        P(("dp", "seq"), None),
        P(),
        P(),
        P(),
        P(),
        P(),
        P(),
        P(),
        P(),
        P(("dp", "seq"), None, None),
        P(("dp", "seq"), None, None),
    )
    return jax.shard_map(
        functools.partial(local, physical_axes(mesh)),
        mesh=mesh,
        in_specs=placed,
        out_specs=(
            P(("dp", "seq"), None, None),
            P(("dp", "seq"), None, None),
            P("dp", "seq", None),
            P(("dp", "seq"), None, None),
            P(),
            P(),
            P(),
            P(),
            P(),
            P(),
            P(),
            P(),
            P(),
        ),
        check_vma=False,
    )
```

```python
import functools

import jax
import jax.numpy as jnp
from jax import lax
from jax.experimental import pallas as pl
from jax.experimental.pallas import tpu as pltpu
from jax.sharding import PartitionSpec as P

HEADS = 12
VOCAB = 24
LONG_REACH = 256

epsilon = 1e-05
blocked = -1e30


def project(matrix, weight):
    return jnp.dot(matrix, weight, preferred_element_type=jnp.float32)


def outer_sum(first_op, second_op):
    return lax.dot_general(
        first_op, second_op, (((0,), (0,)), ((), ())), preferred_element_type=jnp.float32
    )


def against(matrix, weight):
    return lax.dot_general(
        matrix, weight, (((1,), (1,)), ((), ())), preferred_element_type=jnp.float32
    )


def normalize(residual, gain_row, shift_row):
    centered = residual - jnp.mean(residual, -1, keepdims=True)
    factor = lax.rsqrt(jnp.mean(centered * centered, -1, keepdims=True) + epsilon)
    normed = centered * factor
    return (normed * gain_row + shift_row, normed, factor)


def normalize_back(upward, normed, factor, gain_row):
    scaled = upward * gain_row
    result = factor * (
        scaled
        - jnp.mean(scaled, -1, keepdims=True)
        - normed * jnp.mean(scaled * normed, -1, keepdims=True)
    )
    return (result, jnp.sum(upward * normed, 0), jnp.sum(upward, 0))


def blocks_of(long_len, short_len, short_rows):
    step = 128
    found = []
    for start in range(0, long_len, step):
        low = max(0, (start - LONG_REACH + 1) // step * step)
        high = min(long_len, -(-(start + step + LONG_REACH - 1) // step) * step)
        found.append((start, step, low, high, 0, 0))
    for row in range(short_rows):
        base = long_len + row * short_len
        found.append((base, short_len, base, base + short_len, base, row + 1))
    return found


def fill_bias(col_ref, row_ref, long_bias, short_bias, long_len, short_len, short_rows):
    col = col_ref[0:long_len, :]
    row = row_ref[0:1, 0:long_len]
    long_bias[...] = jnp.where(col == row, 0.0, blocked)
    for index in range(short_rows):
        base = long_len + index * short_len
        col = col_ref[base : base + short_len, :]
        row = row_ref[1 + index : 2 + index, 0:short_len]
        short_bias[index] = jnp.where(col == row, 0.0, blocked)


def bias_at(long_bias, short_bias, first, first_count, low, high, base, index):
    if index == 0:
        return long_bias[first : first + first_count, low:high]
    return short_bias[index - 1]


def two_heads(block, lanes, scale):
    half = block.shape[1] // 2
    zero = jnp.zeros_like(block)
    if scale != 1.0:
        block = block * scale
    return jnp.concatenate(
        [jnp.where(lanes < half, block, zero), jnp.where(lanes < half, zero, block)], 0
    )


def attend_kernel(sizes, scale, q_ref, k_ref, v_ref, col_ref, row_ref, o_ref, long_bias, short_bias):
    @pl.when(pl.program_id(0) == 0)
    def _():
        fill_bias(col_ref, row_ref, long_bias, short_bias, *sizes)

    for first, count, low, high, base, index in blocks_of(*sizes):
        lanes = lax.broadcasted_iota(jnp.int32, (count, 128), 1)
        pair = two_heads(q_ref[first : first + count, :], lanes, scale)
        scores = against(pair, k_ref[low:high, :])
        bias = bias_at(long_bias, short_bias, first, count, low, high, base, index)
        scores = scores + jnp.concatenate([bias, bias], 0)
        highest = jnp.max(scores, -1, keepdims=True)
        weights = jnp.exp(scores - highest)
        summed = jnp.sum(weights, -1, keepdims=True)
        mixed = project(weights.astype(jnp.bfloat16), v_ref[low:high, :]) / summed
        o_ref[first : first + count, :] = jnp.where(
            lanes < 64, mixed[:count], mixed[count:]
        ).astype(jnp.bfloat16)


def attend_back_kernel(
    sizes,
    scale,
    q_ref,
    k_ref,
    v_ref,
    g_ref,
    col_ref,
    row_ref,
    dq_ref,
    dk_ref,
    dv_ref,
    long_bias,
    short_bias,
    k_sum,
    v_sum,
):
    @pl.when(pl.program_id(0) == 0)
    def _():
        fill_bias(col_ref, row_ref, long_bias, short_bias, *sizes)

    k_sum[...] = jnp.zeros_like(k_sum)
    v_sum[...] = jnp.zeros_like(v_sum)
    for first, count, low, high, base, index in blocks_of(*sizes):
        lanes = lax.broadcasted_iota(jnp.int32, (count, 128), 1)
        pair = two_heads(q_ref[first : first + count, :], lanes, scale)
        upward = two_heads(g_ref[first : first + count, :], lanes, 1.0)
        keys = k_ref[low:high, :]
        scores = against(keys, pair)
        if index == 0:
            bias = long_bias[low:high, first : first + count]
        else:
            bias = short_bias[index - 1]
        scores = scores + jnp.concatenate([bias, bias], 1)
        highest = jnp.max(scores, 0, keepdims=True)
        weights = jnp.exp(scores - highest)
        weights = weights * (1.0 / jnp.sum(weights, 0, keepdims=True))
        weight_grad = against(v_ref[low:high, :], upward)
        delta = jnp.sum(weights * weight_grad, 0, keepdims=True)
        score_grad = (weights * (weight_grad - delta)).astype(jnp.bfloat16)
        v_sum[low:high, :] += project(weights.astype(jnp.bfloat16), upward)
        k_sum[low:high, :] += project(score_grad, pair)
        q_part = outer_sum(score_grad, keys) * scale
        dq_ref[first : first + count, :] = jnp.where(lanes < 64, q_part[:count], q_part[count:]).astype(
            jnp.bfloat16
        )
    dk_ref[...] = k_sum[...].astype(jnp.bfloat16)
    dv_ref[...] = v_sum[...].astype(jnp.bfloat16)


def attention_calls(sizes, rows, width, scale):
    long_len, short_len, short_rows = sizes
    pairs = width // 128
    column = pl.BlockSpec((rows, 128), lambda i: (0, i))
    col_spec = pl.BlockSpec((rows, 1), lambda i: (0, 0))
    row_spec = pl.BlockSpec((1 + short_rows, long_len), lambda i: (0, 0))
    shape = jax.ShapeDtypeStruct((rows, width), jnp.bfloat16)
    bias = [
        pltpu.VMEM((long_len, long_len), jnp.float32),
        pltpu.VMEM((short_rows, short_len, short_len), jnp.float32),
    ]
    forward = pl.pallas_call(
        functools.partial(attend_kernel, sizes, scale),
        grid=(pairs,),
        in_specs=[column] * 3 + [col_spec, row_spec],
        out_specs=column,
        out_shape=shape,
        scratch_shapes=bias,
        name="attend",
    )
    backward = pl.pallas_call(
        functools.partial(attend_back_kernel, sizes, scale),
        grid=(pairs,),
        in_specs=[column] * 4 + [col_spec, row_spec],
        out_specs=[column] * 3,
        out_shape=[shape] * 3,
        scratch_shapes=bias + [pltpu.VMEM((rows, 128), jnp.float32)] * 2,
        name="attend_back",
    )
    return forward, backward


def physical_axes(mesh):
    first = mesh.devices[0, 0]
    found = {}
    for place, name in enumerate(("x", "y", "z", "core")):

        def at(device):
            return device.core_on_chip if name == "core" else device.coords[place]

        for axis, line in (("dp", mesh.devices[:, 0]), ("seq", mesh.devices[0, :])):
            values = [at(device) - at(first) for device in line]
            size = max(values) + 1
            if size > 1:
                stride = values.index(1)
                assert values == [i // stride % size for i in range(len(values))]
                found[name] = (axis, stride, size)
    return found


def reduce_kernel(axes, orders, chunks, up_ref, down_ref, square_ref, small_ref, token_ref, full, small_out, back, buf, *scratch):
    colors, rows, width = buf.shape
    depth = len(orders[0])
    lands = scratch[:depth]
    small_land, load_sem, send_sem, recv_sem, small_send, small_recv, back_send, back_recv = scratch[depth:]
    chunk = rows // chunks
    spots = {
        name: lax.rem(lax.axis_index(axis) // stride, size)
        for name, (axis, stride, size) in axes.items()
    }

    def peer(name, change):
        axis, stride, size = axes[name]
        target = {other: lax.axis_index(other) for other in ("dp", "seq")}
        target[axis] = target[axis] + change * stride
        return (target["dp"], target["seq"])

    loads = []
    for block in range(up_ref.shape[1] // width):
        loads.append((up_ref.at[:, block * width : (block + 1) * width], buf.at[0, block * width : (block + 1) * width]))
    loads.append((down_ref, buf.at[1]))
    loads.append((square_ref, buf.at[2]))
    copies = [
        pltpu.make_async_copy(source, target, load_sem.at[i]) for i, (source, target) in enumerate(loads)
    ]
    for copy in copies:
        copy.start()

    barrier = pltpu.get_barrier_semaphore()
    greeted = 0
    for name, (axis, stride, size) in axes.items():
        for step in range(1, size):
            change = lax.rem(spots[name] + step, size) - spots[name]
            pl.semaphore_signal(
                barrier, inc=1, device_id=peer(name, change), device_id_type=pl.DeviceIdType.MESH
            )
            greeted += 1
    groups, piece = back.shape[:2]
    here, group = lax.axis_index("seq"), lax.axis_index("dp")
    for step in range(1, groups):
        other = lax.rem(here + step, groups)
        pl.semaphore_signal(
            barrier, inc=1, device_id=(group, other), device_id_type=pl.DeviceIdType.MESH
        )
        greeted += 1
    pl.semaphore_wait(barrier, greeted)
    returns = []
    for step in range(1, groups):
        other = lax.rem(here + step, groups)
        returns.append(
            pltpu.make_async_remote_copy(
                src_ref=token_ref.at[pl.ds(pl.multiple_of(other * piece, 16), piece)],
                dst_ref=back.at[here],
                send_sem=back_send.at[step],
                recv_sem=back_recv.at[step],
                device_id=(group, other),
                device_id_type=pl.DeviceIdType.MESH,
            )
        )
        returns[-1].start()
    back[here] = token_ref[pl.ds(pl.multiple_of(here * piece, 16), piece), :]
    for copy in copies:
        copy.wait()

    def message(color, level, phase, way, k, name, source, target, change):
        return pltpu.make_async_remote_copy(
            src_ref=source,
            dst_ref=target,
            send_sem=send_sem.at[color, level, phase, way, k],
            recv_sem=recv_sem.at[color, level, phase, way, k],
            device_id=peer(name, change),
            device_id_type=pl.DeviceIdType.MESH,
        )

    def plan(color, level, k):
        size = chunk >> (level + 1)
        start = k * chunk
        active = None
        for other in range(level):
            name = orders[color][other]
            last = axes[name][2] - 1
            start = start + jnp.where(spots[name] == last, chunk >> (other + 1), 0)
            if last > 1:
                ends = (spots[name] == 0) | (spots[name] == last)
                active = ends if active is None else active & ends
        return size, start, active

    def guarded(condition, active, body):
        pl.when(condition if active is None else condition & active)(body)

    def reduce_slot(color, level, slot, k):
        name = orders[color][level]
        last = axes[name][2] - 1
        size, start, active = plan(color, level, k)
        for way in range(2):
            place = slot if way == 1 else last - slot
            held = buf.at[color, pl.ds(pl.multiple_of(start + way * size, 16), size)]
            spot = k if lands[level].shape[1] < 2 * chunks * size else 2 * k + way
            land = lands[level].at[color, pl.ds(pl.multiple_of(spot * size, 16), size)]
            change = 1 if way == 1 else -1
            copy = message(color, level, 0, way, k, name, held, land, change)

            into = held
            if level == depth - 1 and slot == last:
                into = full.at[color, pl.ds(pl.multiple_of(start + way * size, 16), size)]

            def body(copy=copy, held=held, land=land, into=into):
                if slot > 0:
                    copy.wait_recv()
                    into[...] = (held[...].astype(jnp.float32) + land[...].astype(jnp.float32)).astype(
                        jnp.bfloat16
                    )
                if slot < last:
                    copy.start()

            guarded(spots[name] == place, active, body)

    def spread_slot(color, level, slot, k):
        name = orders[color][level]
        last = axes[name][2] - 1
        size, start, active = plan(color, level, k)
        for way in range(2):
            place = last - slot if way == 1 else slot
            held = full.at[color, pl.ds(pl.multiple_of(start + way * size, 16), size)]
            change = -1 if way == 1 else 1
            copy = message(color, level, 1, way, k, name, held, held, change)

            def body(copy=copy):
                if slot > 0:
                    copy.wait_recv()
                if slot < last:
                    copy.start()

            guarded(spots[name] == place, active, body)

    def sent(color, level, k):
        name = orders[color][level]
        last = axes[name][2] - 1
        size, start, active = plan(color, level, k)
        for way in range(2):
            held = buf.at[color, pl.ds(pl.multiple_of(start + way * size, 16), size)]
            for phase in range(2):
                copy = message(color, level, phase, way, k, name, held, held, 1)
                stays = spots[name] == (last if (way == 1) == (phase == 0) else 0)
                guarded(jnp.logical_not(stays), active, copy.wait_send)

    small_order = tuple(axes)

    def small_copy(level, step):
        name = small_order[level]
        size = axes[name][2]
        change = lax.rem(spots[name] + step, size) - spots[name]
        slot = sum(axes[other][2] for other in small_order[:level])
        return pltpu.make_async_remote_copy(
            src_ref=small_out,
            dst_ref=small_land.at[slot + step],
            send_sem=small_send.at[slot + step],
            recv_sem=small_recv.at[slot + step],
            device_id=peer(name, change),
            device_id_type=pl.DeviceIdType.MESH,
        )

    def small_start(level):
        for step in range(1, axes[small_order[level]][2]):
            small_copy(level, step).start()

    def small_finish(level):
        name = small_order[level]
        size = axes[name][2]
        slot = sum(axes[other][2] for other in small_order[:level])
        for step in range(1, size):
            small_copy(level, step).wait()
        small_land[slot] = small_out[...]
        total = None
        for place in range(size):
            term = small_land[slot + lax.rem(spots[name] - place + size, size)]
            total = term if total is None else total + term
        small_out[...] = total

    small_out[...] = small_ref[...]
    hops = sum(size - 1 for _, _, size in axes.values())

    def tick(t, carry):
        for color in range(colors):
            base = 0
            for level in range(depth):
                last = axes[orders[color][level]][2] - 1
                for slot in range(last + 1):
                    k = t - (base + slot)

                    @pl.when((k >= 0) & (k < chunks))
                    def _(color=color, level=level, slot=slot, k=k):
                        reduce_slot(color, level, slot, k)

                base += last
            for level in reversed(range(depth)):
                last = axes[orders[color][level]][2] - 1
                for slot in range(last + 1):
                    k = t - (base + slot)

                    @pl.when((k >= 0) & (k < chunks))
                    def _(color=color, level=level, slot=slot, k=k):
                        spread_slot(color, level, slot, k)

                base += last
        for level in range(depth):

            @pl.when(t == 2 * level)
            def _(level=level):
                small_start(level)

            @pl.when(t == 2 * level + 1)
            def _(level=level):
                small_finish(level)

        return carry

    lax.fori_loop(0, chunks + 2 * hops, tick, 0)

    def drain(k, carry):
        for color in range(colors):
            for level in range(depth):
                sent(color, level, k)
        return carry

    lax.fori_loop(0, chunks, drain, 0)
    for copy in returns:
        copy.wait()


def reduce_call(axes, up, down, square, small, token, groups):
    rows, width = down.shape
    colors, chunks = 3, 6
    turn = [name for name in ("x", "y", "z") if name in axes]
    first = [name for name in ("core",) if name in axes]
    orders = [first + turn[i:] + turn[:i] for i in range(3)]
    depth = len(orders[0])
    steps = sum(size for _, _, size in axes.values())
    count = up.shape[1] // width + 2
    sems = (colors, depth, 2, 2, chunks)
    lands = [
        rows >> (level + all(axes[order[level]][2] == 2 for order in orders)) for level in range(depth)
    ]
    return pl.pallas_call(
        functools.partial(reduce_kernel, axes, orders, chunks),
        in_specs=[pl.BlockSpec(memory_space=pl.ANY)] * 3 + [pl.BlockSpec(memory_space=pltpu.VMEM)] * 2,
        out_specs=[pl.BlockSpec(memory_space=pltpu.VMEM)] * 3,
        out_shape=[
            jax.ShapeDtypeStruct((colors, rows, width), jnp.bfloat16),
            jax.ShapeDtypeStruct(small.shape, jnp.float32),
            jax.ShapeDtypeStruct((groups, token.shape[0] // groups, width), jnp.bfloat16),
        ],
        scratch_shapes=[pltpu.VMEM((colors, rows, width), jnp.bfloat16)]
        + [pltpu.VMEM((colors, size, width), jnp.bfloat16) for size in lands]
        + [
            pltpu.VMEM((steps,) + small.shape, jnp.float32),
            pltpu.SemaphoreType.DMA((count,)),
            pltpu.SemaphoreType.DMA(sems),
            pltpu.SemaphoreType.DMA(sems),
            pltpu.SemaphoreType.DMA((steps,)),
            pltpu.SemaphoreType.DMA((steps,)),
            pltpu.SemaphoreType.DMA((groups,)),
            pltpu.SemaphoreType.DMA((groups,)),
        ],
        compiler_params=pltpu.CompilerParams(
            collective_id=0, has_side_effects=True, vmem_limit_bytes=60 * 1024 * 1024
        ),
        name="reduce",
    )(up, down, square, small, token)


def tally(predicted, target, segment):
    residues = jnp.arange(VOCAB, dtype=jnp.int32)[None, :]
    live_mask = (segment > 0).reshape(-1, 1)
    predicted = predicted.reshape(-1, 1)
    target = target.reshape(-1, 1)
    predicted_hot = (predicted == residues) & live_mask
    target_hot = (target == residues) & live_mask
    hit_hot = target_hot & (predicted == target)
    return jnp.stack(
        [
            jnp.sum(predicted_hot.astype(jnp.float32), 0),
            jnp.sum(target_hot.astype(jnp.float32), 0),
            jnp.sum(hit_hot.astype(jnp.float32), 0),
        ]
    )


def local(
    axes,
    x_long,
    x_short,
    seg_long,
    seg_short,
    pred_long,
    target_long,
    pred_short,
    target_short,
    query_weight,
    key_weight,
    value_weight,
    out_weight,
    up_weight,
    down_weight,
    vectors,
    up_bias,
    grad_long,
    grad_short,
):
    local_len, width = x_long.shape[1:]
    short_rows, short_len = x_short.shape[:2]
    groups = lax.axis_size("seq")
    position = lax.axis_index("seq")
    row_len = local_len * groups
    rows_here = x_long.shape[0] // groups
    split = rows_here * row_len
    total = split + short_rows * short_len
    sizes = (row_len, short_len, short_rows)
    forward, backward = attention_calls(sizes, total, width, (width // HEADS) ** (-0.5))

    seg_row = lax.dynamic_slice_in_dim(seg_long, position * rows_here, rows_here, 0)
    seg_local = lax.dynamic_slice_in_dim(seg_long, position * local_len, local_len, 1)
    seg_rows = jnp.concatenate(
        [seg_row, jnp.pad(seg_short, ((0, 0), (0, row_len - short_len)), constant_values=-1)], 0
    )
    seg_column = jnp.concatenate([seg_row.reshape(-1, 1), seg_short.reshape(-1, 1)], 0)

    moved = lax.all_to_all(x_long, "seq", split_axis=0, concat_axis=1, tiled=True)
    tokens = jnp.concatenate([moved.reshape(split, width), x_short.reshape(-1, width)], 0)
    queries = (project(tokens, query_weight) + vectors[0]).astype(jnp.bfloat16)
    key_rows = project(tokens, key_weight).astype(jnp.bfloat16)
    value_rows = (project(tokens, value_weight) + vectors[1]).astype(jnp.bfloat16)
    mixture = forward(queries, key_rows, value_rows, seg_column, seg_rows)
    branch = project(mixture, out_weight) + vectors[2]
    hidden, normed_one, factor_one = normalize(
        tokens.astype(jnp.float32) + branch, vectors[4], vectors[5]
    )
    hidden_low = hidden.astype(jnp.bfloat16)
    pre_act = project(hidden_low, up_weight) + up_bias
    activated, gelu_back = jax.vjp(lambda inner: jax.nn.gelu(inner, approximate=False), pre_act)
    act_low = activated.astype(jnp.bfloat16)
    output, normed_two, factor_two = normalize(
        hidden + project(act_low, down_weight) + vectors[3], vectors[6], vectors[7]
    )
    out_long = output[:split].reshape(rows_here, row_len, width)
    out_short = output[split:].reshape(short_rows, short_len, width)
    upstream = jnp.concatenate(
        [grad_long.reshape(split, width), grad_short.reshape(-1, width)], 0
    ).astype(jnp.float32)
    second_grad, gain_two, shift_two = normalize_back(upstream, normed_two, factor_two, vectors[6])
    down_in = second_grad.astype(jnp.bfloat16)
    down_grad = outer_sum(act_low, down_in)
    down_total = jnp.sum(down_in.astype(jnp.float32), 0)
    pre_grad = gelu_back(against(down_in, down_weight))[0].astype(jnp.bfloat16)
    up_grad = outer_sum(hidden_low, pre_grad)
    bias_total = jnp.sum(pre_grad.astype(jnp.float32), 0)
    hidden_grad = second_grad + against(pre_grad, up_weight)
    first_grad, gain_one, shift_one = normalize_back(
        hidden_grad, normed_one, factor_one, vectors[4]
    )
    branch_in = first_grad.astype(jnp.bfloat16)
    out_grad = outer_sum(mixture, branch_in)
    out_total = jnp.sum(branch_in.astype(jnp.float32), 0)
    mixture_grad = against(branch_in, out_weight).astype(jnp.bfloat16)
    query_in, key_in, value_in = backward(
        queries, key_rows, value_rows, mixture_grad, seg_column, seg_rows
    )
    query_grad = outer_sum(tokens, query_in)
    key_grad = outer_sum(tokens, key_in)
    value_grad = outer_sum(tokens, value_in)
    token_grad = (
        first_grad
        + against(query_in, query_weight)
        + against(key_in, key_weight)
        + against(value_in, value_weight)
    )
    back_short = token_grad[split:].reshape(short_rows, short_len, width)
    counts = tally(pred_long, target_long, seg_local) + tally(pred_short, target_short, seg_short)
    small = jnp.concatenate(
        [
            jnp.stack(
                [
                    jnp.sum(query_in.astype(jnp.float32), 0),
                    jnp.sum(value_in.astype(jnp.float32), 0),
                    out_total,
                    down_total,
                    gain_one,
                    shift_one,
                    gain_two,
                    shift_two,
                ]
            ),
            bias_total.reshape(-1, width),
            jnp.pad(counts.reshape(1, -1), ((0, 3), (0, width - counts.size))),
        ],
        0,
    )
    square = jnp.concatenate([query_grad, key_grad, value_grad, out_grad], 0).astype(jnp.bfloat16)
    summed, small, returned = reduce_call(
        axes,
        up_grad.astype(jnp.bfloat16),
        down_grad.astype(jnp.bfloat16),
        square,
        small,
        token_grad[:split].astype(jnp.bfloat16),
        groups,
    )
    back_long = returned.astype(jnp.float32)
    up_total = jnp.concatenate(
        [summed[0, i : i + width].astype(jnp.float32) for i in range(0, up_grad.shape[1], width)], 1
    )
    vector_rows = 8 + up_bias.size // width
    return (
        out_long,
        out_short,
        back_long,
        back_short,
        *(summed[2, i * width : (i + 1) * width].astype(jnp.float32) for i in range(4)),
        up_total,
        summed[1].astype(jnp.float32),
        small[:8],
        small[8:vector_rows].reshape(-1),
        small[vector_rows, : counts.size].reshape(counts.shape).astype(jnp.int32),
    )


def solution(mesh):
    placed = (
        P("dp", "seq", None),
        P(("dp", "seq"), None, None),
        P("dp", None),
        P(("dp", "seq"), None),
        P("dp", "seq"),
        P("dp", "seq"),
        P(("dp", "seq"), None),
        P(("dp", "seq"), None),
        P(),
        P(),
        P(),
        P(),
        P(),
        P(),
        P(),
        P(),
        P(("dp", "seq"), None, None),
        P(("dp", "seq"), None, None),
    )
    return jax.shard_map(
        functools.partial(local, physical_axes(mesh)),
        mesh=mesh,
        in_specs=placed,
        out_specs=(
            P(("dp", "seq"), None, None),
            P(("dp", "seq"), None, None),
            P("dp", "seq", None),
            P(("dp", "seq"), None, None),
            P(),
            P(),
            P(),
            P(),
            P(),
            P(),
            P(),
            P(),
            P(),
        ),
        check_vma=False,
    )
```

```python
import functools

import jax
import jax.numpy as jnp
from jax import lax
from jax.experimental import pallas as pl
from jax.experimental.pallas import tpu as pltpu
from jax.sharding import PartitionSpec as P

HEADS = 12
VOCAB = 24
LONG_REACH = 256
CHUNKS = 6

epsilon = 1e-05
blocked = -1e30

TAIL = 0.35
SERIES = (
    0.19746604993055228,
    0.19748153788075967,
    0.18507424716028212,
    0.16421743944194458,
    0.10898740989992088,
    0.15459434424968818,
    -0.10693179193342305,
    0.23918706732681347,
    -0.18270557340639457,
    0.042629254353689805,
)


def project(matrix, weight):
    return jnp.dot(matrix, weight, preferred_element_type=jnp.float32)


def outer_sum(first_op, second_op):
    return lax.dot_general(
        first_op, second_op, (((0,), (0,)), ((), ())), preferred_element_type=jnp.float32
    )


def against(matrix, weight):
    return lax.dot_general(
        matrix, weight, (((1,), (1,)), ((), ())), preferred_element_type=jnp.float32
    )


def normalize(residual, gain_row, shift_row):
    centered = residual - jnp.mean(residual, -1, keepdims=True)
    factor = lax.rsqrt(jnp.mean(centered * centered, -1, keepdims=True) + epsilon)
    normed = centered * factor
    return (normed * gain_row + shift_row, normed, factor)


def normalize_back(upward, normed, factor, gain_row):
    scaled = upward * gain_row
    result = factor * (
        scaled
        - jnp.mean(scaled, -1, keepdims=True)
        - normed * jnp.mean(scaled * normed, -1, keepdims=True)
    )
    return (result, jnp.sum(upward * normed, 0), jnp.sum(upward, 0))


def blocks_of(long_len, short_len, short_rows):
    step = 128
    found = []
    for start in range(0, long_len, step):
        low = max(0, (start - LONG_REACH + 1) // step * step)
        high = min(long_len, -(-(start + step + LONG_REACH - 1) // step) * step)
        found.append((start, step, low, high, 0, 0))
    for row in range(short_rows):
        base = long_len + row * short_len
        found.append((base, short_len, base, base + short_len, base, row + 1))
    return found


def fill_bias(col_ref, row_ref, long_bias, short_bias, long_len, short_len, short_rows):
    col = col_ref[0:long_len, :]
    row = row_ref[0:1, 0:long_len]
    long_bias[...] = jnp.where(col == row, 0.0, blocked)
    for index in range(short_rows):
        base = long_len + index * short_len
        col = col_ref[base : base + short_len, :]
        row = row_ref[1 + index : 2 + index, 0:short_len]
        short_bias[index] = jnp.where(col == row, 0.0, blocked)


def bias_at(long_bias, short_bias, first, first_count, low, high, base, index):
    if index == 0:
        return long_bias[first : first + first_count, low:high]
    return short_bias[index - 1]


def two_heads(block, lanes, scale):
    half = block.shape[1] // 2
    zero = jnp.zeros_like(block)
    if scale != 1.0:
        block = block * scale
    return jnp.concatenate(
        [jnp.where(lanes < half, block, zero), jnp.where(lanes < half, zero, block)], 0
    )


def attend_kernel(sizes, scale, q_ref, k_ref, v_ref, col_ref, row_ref, o_ref, long_bias, short_bias):
    @pl.when(pl.program_id(0) == 0)
    def _():
        fill_bias(col_ref, row_ref, long_bias, short_bias, *sizes)

    for first, count, low, high, base, index in blocks_of(*sizes):
        lanes = lax.broadcasted_iota(jnp.int32, (count, 128), 1)
        pair = two_heads(q_ref[first : first + count, :], lanes, scale)
        scores = against(pair, k_ref[low:high, :])
        bias = bias_at(long_bias, short_bias, first, count, low, high, base, index)
        scores = scores + jnp.concatenate([bias, bias], 0)
        highest = jnp.max(scores, -1, keepdims=True)
        weights = jnp.exp(scores - highest)
        summed = jnp.sum(weights, -1, keepdims=True)
        mixed = project(weights.astype(jnp.bfloat16), v_ref[low:high, :]) / summed
        o_ref[first : first + count, :] = jnp.where(
            lanes < 64, mixed[:count], mixed[count:]
        ).astype(jnp.bfloat16)


def attend_back_kernel(
    sizes,
    scale,
    q_ref,
    k_ref,
    v_ref,
    g_ref,
    col_ref,
    row_ref,
    dq_ref,
    dk_ref,
    dv_ref,
    long_bias,
    short_bias,
    k_sum,
    v_sum,
):
    @pl.when(pl.program_id(0) == 0)
    def _():
        fill_bias(col_ref, row_ref, long_bias, short_bias, *sizes)

    k_sum[...] = jnp.zeros_like(k_sum)
    v_sum[...] = jnp.zeros_like(v_sum)
    for first, count, low, high, base, index in blocks_of(*sizes):
        lanes = lax.broadcasted_iota(jnp.int32, (count, 128), 1)
        pair = two_heads(q_ref[first : first + count, :], lanes, scale)
        upward = two_heads(g_ref[first : first + count, :], lanes, 1.0)
        keys = k_ref[low:high, :]
        scores = against(keys, pair)
        if index == 0:
            bias = long_bias[low:high, first : first + count]
        else:
            bias = short_bias[index - 1]
        scores = scores + jnp.concatenate([bias, bias], 1)
        highest = jnp.max(scores, 0, keepdims=True)
        weights = jnp.exp(scores - highest)
        weights = weights * (1.0 / jnp.sum(weights, 0, keepdims=True))
        weight_grad = against(v_ref[low:high, :], upward)
        delta = jnp.sum(weights * weight_grad, 0, keepdims=True)
        score_grad = (weights * (weight_grad - delta)).astype(jnp.bfloat16)
        v_sum[low:high, :] += project(weights.astype(jnp.bfloat16), upward)
        k_sum[low:high, :] += project(score_grad, pair)
        q_part = outer_sum(score_grad, keys) * scale
        dq_ref[first : first + count, :] = jnp.where(lanes < 64, q_part[:count], q_part[count:]).astype(
            jnp.bfloat16
        )
    dk_ref[...] = k_sum[...].astype(jnp.bfloat16)
    dv_ref[...] = v_sum[...].astype(jnp.bfloat16)


def attention_calls(sizes, rows, width, scale):
    long_len, short_len, short_rows = sizes
    pairs = width // 128
    column = pl.BlockSpec((rows, 128), lambda i: (0, i))
    col_spec = pl.BlockSpec((rows, 1), lambda i: (0, 0))
    row_spec = pl.BlockSpec((1 + short_rows, long_len), lambda i: (0, 0))
    shape = jax.ShapeDtypeStruct((rows, width), jnp.bfloat16)
    bias = [
        pltpu.VMEM((long_len, long_len), jnp.float32),
        pltpu.VMEM((short_rows, short_len, short_len), jnp.float32),
    ]
    forward = pl.pallas_call(
        functools.partial(attend_kernel, sizes, scale),
        grid=(pairs,),
        in_specs=[column] * 3 + [col_spec, row_spec],
        out_specs=column,
        out_shape=shape,
        scratch_shapes=bias,
        name="attend",
    )
    backward = pl.pallas_call(
        functools.partial(attend_back_kernel, sizes, scale),
        grid=(pairs,),
        in_specs=[column] * 4 + [col_spec, row_spec],
        out_specs=[column] * 3,
        out_shape=[shape] * 3,
        scratch_shapes=bias + [pltpu.VMEM((rows, 128), jnp.float32)] * 2,
        name="attend_back",
    )
    return forward, backward


def gelu_pair(value):
    size = jnp.abs(value)
    part = 1.0 / (1.0 + size * (TAIL * 0.5**0.5))
    series = SERIES[-1]
    for term in SERIES[-2::-1]:
        series = series * part + term
    bell = jnp.exp(value * value * -0.5)
    tail = (0.5 * part) * series * bell
    share = jnp.where(value < 0.0, tail, 1.0 - tail)
    return value * share, share + value * (bell * 0.3989422804014327)


def up_kernel(strips, h_ref, w_ref, b_ref, act_ref, slope_ref):
    rows = h_ref.shape[0] // strips
    for strip in range(strips):
        span = slice(strip * rows, (strip + 1) * rows)
        value = project(h_ref[span, :], w_ref[...]) + b_ref[...]
        act, slope = gelu_pair(value)
        act_ref[span, :] = act.astype(jnp.bfloat16)
        slope_ref[span, :] = slope.astype(jnp.bfloat16)


def down_back_kernel(strips, g_ref, w_ref, slope_ref, out_ref, sum_ref):
    rows = g_ref.shape[0] // strips
    total = jnp.zeros(sum_ref.shape, jnp.float32)
    for strip in range(strips):
        span = slice(strip * rows, (strip + 1) * rows)
        value = against(g_ref[span, :], w_ref[...]) * slope_ref[span, :].astype(jnp.float32)
        low = value.astype(jnp.bfloat16)
        out_ref[span, :] = low
        total += jnp.sum(low.astype(jnp.float32), 0, keepdims=True)
    sum_ref[...] = total


def feed_calls(rows, width, hidden):
    block, strips = 512, 4
    whole = pl.BlockSpec((rows, width), lambda i: (0, 0))
    column = pl.BlockSpec((rows, block), lambda i: (0, i))
    line = pl.BlockSpec((1, block), lambda i: (0, i))
    shape = jax.ShapeDtypeStruct((rows, hidden), jnp.bfloat16)
    up = pl.pallas_call(
        functools.partial(up_kernel, strips),
        grid=(hidden // block,),
        in_specs=[whole, pl.BlockSpec((width, block), lambda i: (0, i)), line],
        out_specs=[column] * 2,
        out_shape=[shape] * 2,
        name="up",
    )
    down_back = pl.pallas_call(
        functools.partial(down_back_kernel, strips),
        grid=(hidden // block,),
        in_specs=[whole, pl.BlockSpec((block, width), lambda i: (i, 0)), column],
        out_specs=[column, line],
        out_shape=[shape, jax.ShapeDtypeStruct((1, hidden), jnp.float32)],
        name="down_back",
    )
    return up, down_back


def physical_axes(mesh):
    first = mesh.devices[0, 0]
    found = {}
    for place, name in enumerate(("x", "y", "z", "core")):

        def at(device):
            return device.core_on_chip if name == "core" else device.coords[place]

        for axis, line in (("dp", mesh.devices[:, 0]), ("seq", mesh.devices[0, :])):
            values = [at(device) - at(first) for device in line]
            size = max(values) + 1
            if size > 1:
                stride = values.index(1)
                assert values == [i // stride % size for i in range(len(values))]
                found[name] = (axis, stride, size)
    return found


def reduce_kernel(axes, orders, chunks, up_ref, down_ref, q_ref, k_ref, v_ref, o_ref, small_ref, token_ref, full, small_out, back, buf, *scratch):
    colors, rows, width = buf.shape
    depth = len(orders[0])
    lands = scratch[:depth]
    small_land, load_sem, send_sem, recv_sem, small_send, small_recv, back_send, back_recv = scratch[depth:]
    chunk = rows // chunks
    spots = {
        name: lax.rem(lax.axis_index(axis) // stride, size)
        for name, (axis, stride, size) in axes.items()
    }

    def peer(name, change):
        axis, stride, size = axes[name]
        target = {other: lax.axis_index(other) for other in ("dp", "seq")}
        target[axis] = target[axis] + change * stride
        return (target["dp"], target["seq"])

    loads = []
    for block in range(up_ref.shape[1] // width):
        loads.append((up_ref.at[:, block * width : (block + 1) * width], buf.at[0, block * width : (block + 1) * width]))
    loads.append((down_ref, buf.at[1]))
    for block, square in enumerate((q_ref, k_ref, v_ref, o_ref)):
        loads.append((square, buf.at[2, block * width : (block + 1) * width]))
    copies = [
        pltpu.make_async_copy(source, target, load_sem.at[i]) for i, (source, target) in enumerate(loads)
    ]
    for copy in copies:
        copy.start()

    barrier = pltpu.get_barrier_semaphore()
    greeted = 0
    for name, (axis, stride, size) in axes.items():
        for step in range(1, size):
            change = lax.rem(spots[name] + step, size) - spots[name]
            pl.semaphore_signal(
                barrier, inc=1, device_id=peer(name, change), device_id_type=pl.DeviceIdType.MESH
            )
            greeted += 1
    groups, piece = back.shape[:2]
    here, group = lax.axis_index("seq"), lax.axis_index("dp")
    for step in range(1, groups):
        other = lax.rem(here + step, groups)
        pl.semaphore_signal(
            barrier, inc=1, device_id=(group, other), device_id_type=pl.DeviceIdType.MESH
        )
        greeted += 1
    pl.semaphore_wait(barrier, greeted)
    returns = []
    for step in range(1, groups):
        other = lax.rem(here + step, groups)
        returns.append(
            pltpu.make_async_remote_copy(
                src_ref=token_ref.at[pl.ds(pl.multiple_of(other * piece, 16), piece)],
                dst_ref=back.at[here],
                send_sem=back_send.at[step],
                recv_sem=back_recv.at[step],
                device_id=(group, other),
                device_id_type=pl.DeviceIdType.MESH,
            )
        )
        returns[-1].start()
    back[here] = token_ref[pl.ds(pl.multiple_of(here * piece, 16), piece), :]
    for copy in copies:
        copy.wait()

    def message(color, level, phase, way, k, name, source, target, change):
        return pltpu.make_async_remote_copy(
            src_ref=source,
            dst_ref=target,
            send_sem=send_sem.at[color, level, phase, way, k],
            recv_sem=recv_sem.at[color, level, phase, way, k],
            device_id=peer(name, change),
            device_id_type=pl.DeviceIdType.MESH,
        )

    def plan(color, level, k):
        size = chunk >> (level + 1)
        start = k * chunk
        active = None
        for other in range(level):
            name = orders[color][other]
            last = axes[name][2] - 1
            start = start + jnp.where(spots[name] == last, chunk >> (other + 1), 0)
            if last > 1:
                ends = (spots[name] == 0) | (spots[name] == last)
                active = ends if active is None else active & ends
        return size, start, active

    def guarded(condition, active, body):
        pl.when(condition if active is None else condition & active)(body)

    def reduce_slot(color, level, slot, k):
        name = orders[color][level]
        last = axes[name][2] - 1
        size, start, active = plan(color, level, k)
        for way in range(2):
            place = slot if way == 1 else last - slot
            held = buf.at[color, pl.ds(pl.multiple_of(start + way * size, 16), size)]
            spot = k if lands[level].shape[1] < 2 * chunks * size else 2 * k + way
            land = lands[level].at[color, pl.ds(pl.multiple_of(spot * size, 16), size)]
            change = 1 if way == 1 else -1
            copy = message(color, level, 0, way, k, name, held, land, change)

            into = held
            if level == depth - 1 and slot == last:
                into = full.at[color, pl.ds(pl.multiple_of(start + way * size, 16), size)]

            def body(copy=copy, held=held, land=land, into=into):
                if slot > 0:
                    copy.wait_recv()
                    into[...] = (held[...].astype(jnp.float32) + land[...].astype(jnp.float32)).astype(
                        jnp.bfloat16
                    )
                if slot < last:
                    copy.start()

            guarded(spots[name] == place, active, body)

    def spread_slot(color, level, slot, k):
        name = orders[color][level]
        last = axes[name][2] - 1
        size, start, active = plan(color, level, k)
        for way in range(2):
            place = last - slot if way == 1 else slot
            held = full.at[color, pl.ds(pl.multiple_of(start + way * size, 16), size)]
            change = -1 if way == 1 else 1
            copy = message(color, level, 1, way, k, name, held, held, change)

            def body(copy=copy):
                if slot > 0:
                    copy.wait_recv()
                if slot < last:
                    copy.start()

            guarded(spots[name] == place, active, body)

    def sent(color, level, k):
        name = orders[color][level]
        last = axes[name][2] - 1
        size, start, active = plan(color, level, k)
        for way in range(2):
            held = buf.at[color, pl.ds(pl.multiple_of(start + way * size, 16), size)]
            for phase in range(2):
                copy = message(color, level, phase, way, k, name, held, held, 1)
                stays = spots[name] == (last if (way == 1) == (phase == 0) else 0)
                guarded(jnp.logical_not(stays), active, copy.wait_send)

    small_order = tuple(axes)

    def small_copy(level, step):
        name = small_order[level]
        size = axes[name][2]
        change = lax.rem(spots[name] + step, size) - spots[name]
        slot = sum(axes[other][2] for other in small_order[:level])
        return pltpu.make_async_remote_copy(
            src_ref=small_out,
            dst_ref=small_land.at[slot + step],
            send_sem=small_send.at[slot + step],
            recv_sem=small_recv.at[slot + step],
            device_id=peer(name, change),
            device_id_type=pl.DeviceIdType.MESH,
        )

    def small_start(level):
        for step in range(1, axes[small_order[level]][2]):
            small_copy(level, step).start()

    def small_finish(level):
        name = small_order[level]
        size = axes[name][2]
        slot = sum(axes[other][2] for other in small_order[:level])
        for step in range(1, size):
            small_copy(level, step).wait()
        small_land[slot] = small_out[...]
        total = None
        for place in range(size):
            term = small_land[slot + lax.rem(spots[name] - place + size, size)]
            total = term if total is None else total + term
        small_out[...] = total

    small_out[...] = small_ref[...]
    hops = sum(size - 1 for _, _, size in axes.values())

    work = []
    for color in range(colors):
        base = 0
        for spread in (False, True):
            for level in reversed(range(depth)) if spread else range(depth):
                last = axes[orders[color][level]][2] - 1
                for slot in range(last + 1):
                    work.append((abs(base + slot - hops), base + slot, color, spread, level, slot))
                base += last
    work.sort(key=lambda item: item[:3])

    def tick(t, carry):
        for _, offset, color, spread, level, slot in work:
            k = t - offset

            @pl.when((k >= 0) & (k < chunks))
            def _(color=color, spread=spread, level=level, slot=slot, k=k):
                (spread_slot if spread else reduce_slot)(color, level, slot, k)

        for level in range(depth):

            @pl.when(t == 2 * level)
            def _(level=level):
                small_start(level)

            @pl.when(t == 2 * level + 1)
            def _(level=level):
                small_finish(level)

        return carry

    lax.fori_loop(0, chunks + 2 * hops, tick, 0)

    def drain(k, carry):
        for color in range(colors):
            for level in range(depth):
                sent(color, level, k)
        return carry

    lax.fori_loop(0, chunks, drain, 0)
    for copy in returns:
        copy.wait()


def reduce_call(axes, up, down, squares, small, token, groups):
    rows, width = down.shape
    colors, chunks = 3, CHUNKS
    turn = [name for name in ("x", "y", "z") if name in axes]
    first = [name for name in ("core",) if name in axes]
    orders = [first + turn[i:] + turn[:i] for i in range(3)]
    depth = len(orders[0])
    steps = sum(size for _, _, size in axes.values())
    count = up.shape[1] // width + 5
    sems = (colors, depth, 2, 2, chunks)
    lands = [
        rows >> (level + all(axes[order[level]][2] == 2 for order in orders)) for level in range(depth)
    ]
    return pl.pallas_call(
        functools.partial(reduce_kernel, axes, orders, chunks),
        in_specs=[pl.BlockSpec(memory_space=pl.ANY)] * 6 + [pl.BlockSpec(memory_space=pltpu.VMEM)] * 2,
        out_specs=[pl.BlockSpec(memory_space=pltpu.VMEM)] * 3,
        out_shape=[
            jax.ShapeDtypeStruct((colors, rows, width), jnp.bfloat16),
            jax.ShapeDtypeStruct(small.shape, jnp.float32),
            jax.ShapeDtypeStruct((groups, token.shape[0] // groups, width), jnp.bfloat16),
        ],
        scratch_shapes=[pltpu.VMEM((colors, rows, width), jnp.bfloat16)]
        + [pltpu.VMEM((colors, size, width), jnp.bfloat16) for size in lands]
        + [
            pltpu.VMEM((steps,) + small.shape, jnp.float32),
            pltpu.SemaphoreType.DMA((count,)),
            pltpu.SemaphoreType.DMA(sems),
            pltpu.SemaphoreType.DMA(sems),
            pltpu.SemaphoreType.DMA((steps,)),
            pltpu.SemaphoreType.DMA((steps,)),
            pltpu.SemaphoreType.DMA((groups,)),
            pltpu.SemaphoreType.DMA((groups,)),
        ],
        compiler_params=pltpu.CompilerParams(
            collective_id=0, has_side_effects=True, vmem_limit_bytes=60 * 1024 * 1024
        ),
        name="reduce",
    )(up, down, *squares, small, token)


def tally(predicted, target, segment):
    residues = jnp.arange(VOCAB, dtype=jnp.int32)[None, :]
    live_mask = (segment > 0).reshape(-1, 1)
    predicted = predicted.reshape(-1, 1)
    target = target.reshape(-1, 1)
    predicted_hot = (predicted == residues) & live_mask
    target_hot = (target == residues) & live_mask
    hit_hot = target_hot & (predicted == target)
    return jnp.stack(
        [
            jnp.sum(predicted_hot.astype(jnp.float32), 0),
            jnp.sum(target_hot.astype(jnp.float32), 0),
            jnp.sum(hit_hot.astype(jnp.float32), 0),
        ]
    )


def local(
    axes,
    x_long,
    x_short,
    seg_long,
    seg_short,
    pred_long,
    target_long,
    pred_short,
    target_short,
    query_weight,
    key_weight,
    value_weight,
    out_weight,
    up_weight,
    down_weight,
    vectors,
    up_bias,
    grad_long,
    grad_short,
):
    local_len, width = x_long.shape[1:]
    short_rows, short_len = x_short.shape[:2]
    groups = lax.axis_size("seq")
    position = lax.axis_index("seq")
    row_len = local_len * groups
    rows_here = x_long.shape[0] // groups
    split = rows_here * row_len
    total = split + short_rows * short_len
    sizes = (row_len, short_len, short_rows)
    forward, backward = attention_calls(sizes, total, width, (width // HEADS) ** (-0.5))

    seg_row = lax.dynamic_slice_in_dim(seg_long, position * rows_here, rows_here, 0)
    seg_local = lax.dynamic_slice_in_dim(seg_long, position * local_len, local_len, 1)
    seg_rows = jnp.concatenate(
        [seg_row, jnp.pad(seg_short, ((0, 0), (0, row_len - short_len)), constant_values=-1)], 0
    )
    seg_column = jnp.concatenate([seg_row.reshape(-1, 1), seg_short.reshape(-1, 1)], 0)

    moved = lax.all_to_all(x_long, "seq", split_axis=0, concat_axis=1, tiled=True)
    tokens = jnp.concatenate([moved.reshape(split, width), x_short.reshape(-1, width)], 0)
    queries = (project(tokens, query_weight) + vectors[0]).astype(jnp.bfloat16)
    key_rows = project(tokens, key_weight).astype(jnp.bfloat16)
    value_rows = (project(tokens, value_weight) + vectors[1]).astype(jnp.bfloat16)
    mixture = forward(queries, key_rows, value_rows, seg_column, seg_rows)
    branch = project(mixture, out_weight) + vectors[2]
    hidden, normed_one, factor_one = normalize(
        tokens.astype(jnp.float32) + branch, vectors[4], vectors[5]
    )
    hidden_low = hidden.astype(jnp.bfloat16)
    up_call, down_back_call = feed_calls(total, width, up_bias.size)
    act_low, slope = up_call(hidden_low, up_weight, up_bias.reshape(1, -1))
    output, normed_two, factor_two = normalize(
        hidden + project(act_low, down_weight) + vectors[3], vectors[6], vectors[7]
    )
    out_long = output[:split].reshape(rows_here, row_len, width)
    out_short = output[split:].reshape(short_rows, short_len, width)
    upstream = jnp.concatenate(
        [grad_long.reshape(split, width), grad_short.reshape(-1, width)], 0
    ).astype(jnp.float32)
    second_grad, gain_two, shift_two = normalize_back(upstream, normed_two, factor_two, vectors[6])
    down_in = second_grad.astype(jnp.bfloat16)
    down_grad = outer_sum(act_low, down_in)
    down_total = jnp.sum(down_in.astype(jnp.float32), 0)
    pre_grad, bias_total = down_back_call(down_in, down_weight, slope)
    up_grad = outer_sum(hidden_low, pre_grad)
    hidden_grad = second_grad + against(pre_grad, up_weight)
    first_grad, gain_one, shift_one = normalize_back(
        hidden_grad, normed_one, factor_one, vectors[4]
    )
    branch_in = first_grad.astype(jnp.bfloat16)
    out_grad = outer_sum(mixture, branch_in)
    out_total = jnp.sum(branch_in.astype(jnp.float32), 0)
    mixture_grad = against(branch_in, out_weight).astype(jnp.bfloat16)
    query_in, key_in, value_in = backward(
        queries, key_rows, value_rows, mixture_grad, seg_column, seg_rows
    )
    query_grad = outer_sum(tokens, query_in)
    key_grad = outer_sum(tokens, key_in)
    value_grad = outer_sum(tokens, value_in)
    token_grad = (
        first_grad
        + against(query_in, query_weight)
        + against(key_in, key_weight)
        + against(value_in, value_weight)
    )
    back_short = token_grad[split:].reshape(short_rows, short_len, width)
    counts = tally(pred_long, target_long, seg_local) + tally(pred_short, target_short, seg_short)
    small = jnp.concatenate(
        [
            jnp.stack(
                [
                    jnp.sum(query_in.astype(jnp.float32), 0),
                    jnp.sum(value_in.astype(jnp.float32), 0),
                    out_total,
                    down_total,
                    gain_one,
                    shift_one,
                    gain_two,
                    shift_two,
                ]
            ),
            bias_total.reshape(-1, width),
            jnp.pad(counts.reshape(1, -1), ((0, 3), (0, width - counts.size))),
        ],
        0,
    )
    squares = [part.astype(jnp.bfloat16) for part in (query_grad, key_grad, value_grad, out_grad)]
    summed, small, returned = reduce_call(
        axes,
        up_grad.astype(jnp.bfloat16),
        down_grad.astype(jnp.bfloat16),
        squares,
        small,
        token_grad[:split].astype(jnp.bfloat16),
        groups,
    )
    back_long = returned.astype(jnp.float32)
    up_total = jnp.concatenate(
        [summed[0, i : i + width].astype(jnp.float32) for i in range(0, up_grad.shape[1], width)], 1
    )
    vector_rows = 8 + up_bias.size // width
    return (
        out_long,
        out_short,
        back_long,
        back_short,
        *(summed[2, i * width : (i + 1) * width].astype(jnp.float32) for i in range(4)),
        up_total,
        summed[1].astype(jnp.float32),
        small[:8],
        small[8:vector_rows].reshape(-1),
        small[vector_rows, : counts.size].reshape(counts.shape).astype(jnp.int32),
    )


def solution(mesh):
    placed = (
        P("dp", "seq", None),
        P(("dp", "seq"), None, None),
        P("dp", None),
        P(("dp", "seq"), None),
        P("dp", "seq"),
        P("dp", "seq"),
        P(("dp", "seq"), None),
        P(("dp", "seq"), None),
        P(),
        P(),
        P(),
        P(),
        P(),
        P(),
        P(),
        P(),
        P(("dp", "seq"), None, None),
        P(("dp", "seq"), None, None),
    )
    return jax.shard_map(
        functools.partial(local, physical_axes(mesh)),
        mesh=mesh,
        in_specs=placed,
        out_specs=(
            P(("dp", "seq"), None, None),
            P(("dp", "seq"), None, None),
            P("dp", "seq", None),
            P(("dp", "seq"), None, None),
            P(),
            P(),
            P(),
            P(),
            P(),
            P(),
            P(),
            P(),
            P(),
        ),
        check_vma=False,
    )
```

```python
import functools

import jax
import jax.numpy as jnp
from jax import lax
from jax.experimental import pallas as pl
from jax.experimental.pallas import tpu as pltpu
from jax.sharding import PartitionSpec as P

HEADS = 12
VOCAB = 24
LONG_REACH = 256
CHUNKS = 4

epsilon = 1e-05
blocked = -1e30

TAIL = 0.35
SERIES = (
    0.19746604993055228,
    0.19748153788075967,
    0.18507424716028212,
    0.16421743944194458,
    0.10898740989992088,
    0.15459434424968818,
    -0.10693179193342305,
    0.23918706732681347,
    -0.18270557340639457,
    0.042629254353689805,
)


def project(matrix, weight):
    return jnp.dot(matrix, weight, preferred_element_type=jnp.float32)


def outer_sum(first_op, second_op):
    return lax.dot_general(
        first_op, second_op, (((0,), (0,)), ((), ())), preferred_element_type=jnp.float32
    )


def against(matrix, weight):
    return lax.dot_general(
        matrix, weight, (((1,), (1,)), ((), ())), preferred_element_type=jnp.float32
    )


def normalize(residual, gain_row, shift_row):
    centered = residual - jnp.mean(residual, -1, keepdims=True)
    factor = lax.rsqrt(jnp.mean(centered * centered, -1, keepdims=True) + epsilon)
    normed = centered * factor
    return (normed * gain_row + shift_row, normed, factor)


def normalize_back(upward, normed, factor, gain_row):
    scaled = upward * gain_row
    result = factor * (
        scaled
        - jnp.mean(scaled, -1, keepdims=True)
        - normed * jnp.mean(scaled * normed, -1, keepdims=True)
    )
    return (result, jnp.sum(upward * normed, 0), jnp.sum(upward, 0))


def blocks_of(long_len, short_len, short_rows):
    step = 128
    found = []
    for start in range(0, long_len, step):
        low = max(0, (start - LONG_REACH + 1) // step * step)
        high = min(long_len, -(-(start + step + LONG_REACH - 1) // step) * step)
        found.append((start, step, low, high, 0, 0))
    for row in range(short_rows):
        base = long_len + row * short_len
        found.append((base, short_len, base, base + short_len, base, row + 1))
    return found


def fill_bias(col_ref, row_ref, long_bias, short_bias, long_len, short_len, short_rows):
    col = col_ref[0:long_len, :]
    row = row_ref[0:1, 0:long_len]
    long_bias[...] = jnp.where(col == row, 0.0, blocked)
    for index in range(short_rows):
        base = long_len + index * short_len
        col = col_ref[base : base + short_len, :]
        row = row_ref[1 + index : 2 + index, 0:short_len]
        short_bias[index] = jnp.where(col == row, 0.0, blocked)


def bias_at(long_bias, short_bias, first, first_count, low, high, base, index):
    if index == 0:
        return long_bias[first : first + first_count, low:high]
    return short_bias[index - 1]


def two_heads(block, lanes, scale):
    half = block.shape[1] // 2
    zero = jnp.zeros_like(block)
    if scale != 1.0:
        block = block * scale
    return jnp.concatenate(
        [jnp.where(lanes < half, block, zero), jnp.where(lanes < half, zero, block)], 0
    )


def attend_kernel(sizes, scale, q_ref, k_ref, v_ref, col_ref, row_ref, o_ref, long_bias, short_bias):
    @pl.when(pl.program_id(0) == 0)
    def _():
        fill_bias(col_ref, row_ref, long_bias, short_bias, *sizes)

    for first, count, low, high, base, index in blocks_of(*sizes):
        lanes = lax.broadcasted_iota(jnp.int32, (count, 128), 1)
        pair = two_heads(q_ref[first : first + count, :], lanes, scale)
        scores = against(pair, k_ref[low:high, :])
        bias = bias_at(long_bias, short_bias, first, count, low, high, base, index)
        scores = scores + jnp.concatenate([bias, bias], 0)
        highest = jnp.max(scores, -1, keepdims=True)
        weights = jnp.exp(scores - highest)
        summed = jnp.sum(weights, -1, keepdims=True)
        mixed = project(weights.astype(jnp.bfloat16), v_ref[low:high, :]) / summed
        o_ref[first : first + count, :] = jnp.where(
            lanes < 64, mixed[:count], mixed[count:]
        ).astype(jnp.bfloat16)


def attend_back_kernel(
    sizes,
    scale,
    q_ref,
    k_ref,
    v_ref,
    g_ref,
    col_ref,
    row_ref,
    dq_ref,
    dk_ref,
    dv_ref,
    long_bias,
    short_bias,
    k_sum,
    v_sum,
):
    @pl.when(pl.program_id(0) == 0)
    def _():
        fill_bias(col_ref, row_ref, long_bias, short_bias, *sizes)

    k_sum[...] = jnp.zeros_like(k_sum)
    v_sum[...] = jnp.zeros_like(v_sum)
    for first, count, low, high, base, index in blocks_of(*sizes):
        lanes = lax.broadcasted_iota(jnp.int32, (count, 128), 1)
        pair = two_heads(q_ref[first : first + count, :], lanes, scale)
        upward = two_heads(g_ref[first : first + count, :], lanes, 1.0)
        keys = k_ref[low:high, :]
        scores = against(keys, pair)
        if index == 0:
            bias = long_bias[low:high, first : first + count]
        else:
            bias = short_bias[index - 1]
        scores = scores + jnp.concatenate([bias, bias], 1)
        highest = jnp.max(scores, 0, keepdims=True)
        weights = jnp.exp(scores - highest)
        weights = weights * (1.0 / jnp.sum(weights, 0, keepdims=True))
        weight_grad = against(v_ref[low:high, :], upward)
        delta = jnp.sum(weights * weight_grad, 0, keepdims=True)
        score_grad = (weights * (weight_grad - delta)).astype(jnp.bfloat16)
        v_sum[low:high, :] += project(weights.astype(jnp.bfloat16), upward)
        k_sum[low:high, :] += project(score_grad, pair)
        q_part = outer_sum(score_grad, keys) * scale
        dq_ref[first : first + count, :] = jnp.where(lanes < 64, q_part[:count], q_part[count:]).astype(
            jnp.bfloat16
        )
    dk_ref[...] = k_sum[...].astype(jnp.bfloat16)
    dv_ref[...] = v_sum[...].astype(jnp.bfloat16)


def attention_calls(sizes, rows, width, scale):
    long_len, short_len, short_rows = sizes
    pairs = width // 128
    column = pl.BlockSpec((rows, 128), lambda i: (0, i))
    col_spec = pl.BlockSpec((rows, 1), lambda i: (0, 0))
    row_spec = pl.BlockSpec((1 + short_rows, long_len), lambda i: (0, 0))
    shape = jax.ShapeDtypeStruct((rows, width), jnp.bfloat16)
    bias = [
        pltpu.VMEM((long_len, long_len), jnp.float32),
        pltpu.VMEM((short_rows, short_len, short_len), jnp.float32),
    ]
    forward = pl.pallas_call(
        functools.partial(attend_kernel, sizes, scale),
        grid=(pairs,),
        in_specs=[column] * 3 + [col_spec, row_spec],
        out_specs=column,
        out_shape=shape,
        scratch_shapes=bias,
        name="attend",
    )
    backward = pl.pallas_call(
        functools.partial(attend_back_kernel, sizes, scale),
        grid=(pairs,),
        in_specs=[column] * 4 + [col_spec, row_spec],
        out_specs=[column] * 3,
        out_shape=[shape] * 3,
        scratch_shapes=bias + [pltpu.VMEM((rows, 128), jnp.float32)] * 2,
        name="attend_back",
    )
    return forward, backward


def gelu_pair(value):
    size = jnp.abs(value)
    part = 1.0 / (1.0 + size * (TAIL * 0.5**0.5))
    series = SERIES[-1]
    for term in SERIES[-2::-1]:
        series = series * part + term
    bell = jnp.exp(value * value * -0.5)
    tail = (0.5 * part) * series * bell
    share = jnp.where(value < 0.0, tail, 1.0 - tail)
    return value * share, share + value * (bell * 0.3989422804014327)


def up_kernel(strips, h_ref, w_ref, b_ref, act_ref, slope_ref):
    rows = h_ref.shape[0] // strips
    for strip in range(strips):
        span = slice(strip * rows, (strip + 1) * rows)
        value = project(h_ref[span, :], w_ref[...]) + b_ref[...]
        act, slope = gelu_pair(value)
        act_ref[span, :] = act.astype(jnp.bfloat16)
        slope_ref[span, :] = slope.astype(jnp.bfloat16)


def down_back_kernel(strips, g_ref, w_ref, slope_ref, out_ref, sum_ref):
    rows = g_ref.shape[0] // strips
    total = jnp.zeros(sum_ref.shape, jnp.float32)
    for strip in range(strips):
        span = slice(strip * rows, (strip + 1) * rows)
        value = against(g_ref[span, :], w_ref[...]) * slope_ref[span, :].astype(jnp.float32)
        low = value.astype(jnp.bfloat16)
        out_ref[span, :] = low
        total += jnp.sum(low.astype(jnp.float32), 0, keepdims=True)
    sum_ref[...] = total


def feed_calls(rows, width, hidden):
    block, strips = 512, 4
    whole = pl.BlockSpec((rows, width), lambda i: (0, 0))
    column = pl.BlockSpec((rows, block), lambda i: (0, i))
    line = pl.BlockSpec((1, block), lambda i: (0, i))
    shape = jax.ShapeDtypeStruct((rows, hidden), jnp.bfloat16)
    up = pl.pallas_call(
        functools.partial(up_kernel, strips),
        grid=(hidden // block,),
        in_specs=[whole, pl.BlockSpec((width, block), lambda i: (0, i)), line],
        out_specs=[column] * 2,
        out_shape=[shape] * 2,
        name="up",
    )
    down_back = pl.pallas_call(
        functools.partial(down_back_kernel, strips),
        grid=(hidden // block,),
        in_specs=[whole, pl.BlockSpec((block, width), lambda i: (i, 0)), column],
        out_specs=[column, line],
        out_shape=[shape, jax.ShapeDtypeStruct((1, hidden), jnp.float32)],
        name="down_back",
    )
    return up, down_back


def physical_axes(mesh):
    first = mesh.devices[0, 0]
    found = {}
    for place, name in enumerate(("x", "y", "z", "core")):

        def at(device):
            return device.core_on_chip if name == "core" else device.coords[place]

        for axis, line in (("dp", mesh.devices[:, 0]), ("seq", mesh.devices[0, :])):
            values = [at(device) - at(first) for device in line]
            size = max(values) + 1
            if size > 1:
                stride = values.index(1)
                assert values == [i // stride % size for i in range(len(values))]
                found[name] = (axis, stride, size)
    return found


def reduce_kernel(axes, orders, chunks, up_ref, q_ref, k_ref, v_ref, o_ref, small_ref, token_ref, full, small_out, back, buf, *scratch):
    colors, rows, width = buf.shape
    depth = len(orders[0])
    lands = scratch[:depth]
    small_land, load_sem, send_sem, recv_sem, small_send, small_recv, back_send, back_recv = scratch[depth:]
    chunk = rows // chunks
    spots = {
        name: lax.rem(lax.axis_index(axis) // stride, size)
        for name, (axis, stride, size) in axes.items()
    }

    def peer(name, change):
        axis, stride, size = axes[name]
        target = {other: lax.axis_index(other) for other in ("dp", "seq")}
        target[axis] = target[axis] + change * stride
        return (target["dp"], target["seq"])

    pieces = [up_ref.at[:, i : i + width] for i in range(0, up_ref.shape[1], width)]
    loads = []
    for block, piece in enumerate(pieces + [q_ref, k_ref, v_ref, o_ref]):
        first, end = block * width, (block + 1) * width
        while first < end:
            color, stop = first // rows, min(end, (first // rows + 1) * rows)
            source = piece.at[first - block * width : stop - block * width]
            loads.append((source, buf.at[color, first - color * rows : stop - color * rows]))
            first = stop
    copies = [
        pltpu.make_async_copy(source, target, load_sem.at[i]) for i, (source, target) in enumerate(loads)
    ]
    for copy in copies:
        copy.start()

    barrier = pltpu.get_barrier_semaphore()
    greeted = 0
    for name, (axis, stride, size) in axes.items():
        for step in range(1, size):
            change = lax.rem(spots[name] + step, size) - spots[name]
            pl.semaphore_signal(
                barrier, inc=1, device_id=peer(name, change), device_id_type=pl.DeviceIdType.MESH
            )
            greeted += 1
    groups, piece = back.shape[:2]
    here, group = lax.axis_index("seq"), lax.axis_index("dp")
    for step in range(1, groups):
        other = lax.rem(here + step, groups)
        pl.semaphore_signal(
            barrier, inc=1, device_id=(group, other), device_id_type=pl.DeviceIdType.MESH
        )
        greeted += 1
    pl.semaphore_wait(barrier, greeted)
    returns = []
    for step in range(1, groups):
        other = lax.rem(here + step, groups)
        returns.append(
            pltpu.make_async_remote_copy(
                src_ref=token_ref.at[pl.ds(pl.multiple_of(other * piece, 16), piece)],
                dst_ref=back.at[here],
                send_sem=back_send.at[step],
                recv_sem=back_recv.at[step],
                device_id=(group, other),
                device_id_type=pl.DeviceIdType.MESH,
            )
        )
        returns[-1].start()
    back[here] = token_ref[pl.ds(pl.multiple_of(here * piece, 16), piece), :]
    for copy in copies:
        copy.wait()

    def message(color, level, phase, way, k, name, source, target, change):
        return pltpu.make_async_remote_copy(
            src_ref=source,
            dst_ref=target,
            send_sem=send_sem.at[color, level, phase, way, k],
            recv_sem=recv_sem.at[color, level, phase, way, k],
            device_id=peer(name, change),
            device_id_type=pl.DeviceIdType.MESH,
        )

    def plan(color, level, k):
        size = chunk >> (level + 1)
        start = k * chunk
        active = None
        for other in range(level):
            name = orders[color][other]
            last = axes[name][2] - 1
            start = start + jnp.where(spots[name] == last, chunk >> (other + 1), 0)
            if last > 1:
                ends = (spots[name] == 0) | (spots[name] == last)
                active = ends if active is None else active & ends
        return size, start, active

    def guarded(condition, active, body):
        pl.when(condition if active is None else condition & active)(body)

    def reduce_slot(color, level, slot, k):
        name = orders[color][level]
        last = axes[name][2] - 1
        size, start, active = plan(color, level, k)
        for way in range(2):
            place = slot if way == 1 else last - slot
            held = buf.at[color, pl.ds(pl.multiple_of(start + way * size, 16), size)]
            spot = k if lands[level].shape[1] < 2 * chunks * size else 2 * k + way
            land = lands[level].at[color, pl.ds(pl.multiple_of(spot * size, 16), size)]
            change = 1 if way == 1 else -1
            copy = message(color, level, 0, way, k, name, held, land, change)

            into = held
            if level == depth - 1 and slot == last:
                into = full.at[color, pl.ds(pl.multiple_of(start + way * size, 16), size)]

            def body(copy=copy, held=held, land=land, into=into):
                if slot > 0:
                    copy.wait_recv()
                    into[...] = (held[...].astype(jnp.float32) + land[...].astype(jnp.float32)).astype(
                        jnp.bfloat16
                    )
                if slot < last:
                    copy.start()

            guarded(spots[name] == place, active, body)

    def spread_slot(color, level, slot, k):
        name = orders[color][level]
        last = axes[name][2] - 1
        size, start, active = plan(color, level, k)
        for way in range(2):
            place = last - slot if way == 1 else slot
            held = full.at[color, pl.ds(pl.multiple_of(start + way * size, 16), size)]
            change = -1 if way == 1 else 1
            copy = message(color, level, 1, way, k, name, held, held, change)

            def body(copy=copy):
                if slot > 0:
                    copy.wait_recv()
                if slot < last:
                    copy.start()

            guarded(spots[name] == place, active, body)

    def sent(color, level, k):
        name = orders[color][level]
        last = axes[name][2] - 1
        size, start, active = plan(color, level, k)
        for way in range(2):
            held = buf.at[color, pl.ds(pl.multiple_of(start + way * size, 16), size)]
            for phase in range(2):
                copy = message(color, level, phase, way, k, name, held, held, 1)
                stays = spots[name] == (last if (way == 1) == (phase == 0) else 0)
                guarded(jnp.logical_not(stays), active, copy.wait_send)

    small_order = tuple(axes)

    def small_copy(level, step):
        name = small_order[level]
        size = axes[name][2]
        change = lax.rem(spots[name] + step, size) - spots[name]
        slot = sum(axes[other][2] for other in small_order[:level])
        return pltpu.make_async_remote_copy(
            src_ref=small_out,
            dst_ref=small_land.at[slot + step],
            send_sem=small_send.at[slot + step],
            recv_sem=small_recv.at[slot + step],
            device_id=peer(name, change),
            device_id_type=pl.DeviceIdType.MESH,
        )

    def small_start(level):
        for step in range(1, axes[small_order[level]][2]):
            small_copy(level, step).start()

    def small_finish(level):
        name = small_order[level]
        size = axes[name][2]
        slot = sum(axes[other][2] for other in small_order[:level])
        for step in range(1, size):
            small_copy(level, step).wait()
        small_land[slot] = small_out[...]
        total = None
        for place in range(size):
            term = small_land[slot + lax.rem(spots[name] - place + size, size)]
            total = term if total is None else total + term
        small_out[...] = total

    small_out[...] = small_ref[...]
    hops = sum(size - 1 for _, _, size in axes.values())

    work = []
    for color in range(colors):
        base = 0
        for spread in (False, True):
            for level in reversed(range(depth)) if spread else range(depth):
                last = axes[orders[color][level]][2] - 1
                for slot in range(last + 1):
                    work.append((abs(base + slot - hops), base + slot, color, spread, level, slot))
                base += last
    work.sort(key=lambda item: item[:3])

    def tick(t, carry):
        for _, offset, color, spread, level, slot in work:
            k = t - offset

            @pl.when((k >= 0) & (k < chunks))
            def _(color=color, spread=spread, level=level, slot=slot, k=k):
                (spread_slot if spread else reduce_slot)(color, level, slot, k)

        for level in range(depth):

            @pl.when(t == 2 * level)
            def _(level=level):
                small_start(level)

            @pl.when(t == 2 * level + 1)
            def _(level=level):
                small_finish(level)

        return carry

    lax.fori_loop(0, chunks + 2 * hops, tick, 0)

    def drain(k, carry):
        for color in range(colors):
            for level in range(depth):
                sent(color, level, k)
        return carry

    lax.fori_loop(0, chunks, drain, 0)
    for copy in returns:
        copy.wait()


def reduce_call(axes, up, squares, small, token, groups):
    width = up.shape[0]
    colors, chunks = 3, CHUNKS
    rows = (up.shape[1] + 4 * width) // colors
    turn = [name for name in ("x", "y", "z") if name in axes]
    first = [name for name in ("core",) if name in axes]
    orders = [first + turn[i:] + turn[:i] for i in range(3)]
    depth = len(orders[0])
    steps = sum(size for _, _, size in axes.values())
    count = up.shape[1] // width + 4 + colors
    sems = (colors, depth, 2, 2, chunks)
    lands = [
        rows >> (level + all(axes[order[level]][2] == 2 for order in orders)) for level in range(depth)
    ]
    return pl.pallas_call(
        functools.partial(reduce_kernel, axes, orders, chunks),
        in_specs=[pl.BlockSpec(memory_space=pl.ANY)] * 5 + [pl.BlockSpec(memory_space=pltpu.VMEM)] * 2,
        out_specs=[pl.BlockSpec(memory_space=pltpu.VMEM)] * 3,
        out_shape=[
            jax.ShapeDtypeStruct((colors, rows, width), jnp.bfloat16),
            jax.ShapeDtypeStruct(small.shape, jnp.float32),
            jax.ShapeDtypeStruct((groups, token.shape[0] // groups, width), jnp.bfloat16),
        ],
        scratch_shapes=[pltpu.VMEM((colors, rows, width), jnp.bfloat16)]
        + [pltpu.VMEM((colors, size, width), jnp.bfloat16) for size in lands]
        + [
            pltpu.VMEM((steps,) + small.shape, jnp.float32),
            pltpu.SemaphoreType.DMA((count,)),
            pltpu.SemaphoreType.DMA(sems),
            pltpu.SemaphoreType.DMA(sems),
            pltpu.SemaphoreType.DMA((steps,)),
            pltpu.SemaphoreType.DMA((steps,)),
            pltpu.SemaphoreType.DMA((groups,)),
            pltpu.SemaphoreType.DMA((groups,)),
        ],
        compiler_params=pltpu.CompilerParams(
            collective_id=0, has_side_effects=True, vmem_limit_bytes=60 * 1024 * 1024
        ),
        name="reduce",
    )(up, *squares, small, token)


def tally(predicted, target, segment):
    residues = jnp.arange(VOCAB, dtype=jnp.int32)[None, :]
    live_mask = (segment > 0).reshape(-1, 1)
    predicted = predicted.reshape(-1, 1)
    target = target.reshape(-1, 1)
    predicted_hot = (predicted == residues) & live_mask
    target_hot = (target == residues) & live_mask
    hit_hot = target_hot & (predicted == target)
    return jnp.stack(
        [
            jnp.sum(predicted_hot.astype(jnp.float32), 0),
            jnp.sum(target_hot.astype(jnp.float32), 0),
            jnp.sum(hit_hot.astype(jnp.float32), 0),
        ]
    )


def local(
    axes,
    x_long,
    x_short,
    seg_long,
    seg_short,
    pred_long,
    target_long,
    pred_short,
    target_short,
    query_weight,
    key_weight,
    value_weight,
    out_weight,
    up_weight,
    down_weight,
    vectors,
    up_bias,
    grad_long,
    grad_short,
):
    local_len, width = x_long.shape[1:]
    short_rows, short_len = x_short.shape[:2]
    groups = lax.axis_size("seq")
    position = lax.axis_index("seq")
    row_len = local_len * groups
    rows_here = x_long.shape[0] // groups
    split = rows_here * row_len
    total = split + short_rows * short_len
    sizes = (row_len, short_len, short_rows)
    forward, backward = attention_calls(sizes, total, width, (width // HEADS) ** (-0.5))

    seg_row = lax.dynamic_slice_in_dim(seg_long, position * rows_here, rows_here, 0)
    seg_local = lax.dynamic_slice_in_dim(seg_long, position * local_len, local_len, 1)
    seg_rows = jnp.concatenate(
        [seg_row, jnp.pad(seg_short, ((0, 0), (0, row_len - short_len)), constant_values=-1)], 0
    )
    seg_column = jnp.concatenate([seg_row.reshape(-1, 1), seg_short.reshape(-1, 1)], 0)

    moved = lax.all_to_all(x_long, "seq", split_axis=0, concat_axis=1, tiled=True)
    tokens = jnp.concatenate([moved.reshape(split, width), x_short.reshape(-1, width)], 0)
    queries = (project(tokens, query_weight) + vectors[0]).astype(jnp.bfloat16)
    key_rows = project(tokens, key_weight).astype(jnp.bfloat16)
    value_rows = (project(tokens, value_weight) + vectors[1]).astype(jnp.bfloat16)
    mixture = forward(queries, key_rows, value_rows, seg_column, seg_rows)
    branch = project(mixture, out_weight) + vectors[2]
    hidden, normed_one, factor_one = normalize(
        tokens.astype(jnp.float32) + branch, vectors[4], vectors[5]
    )
    hidden_low = hidden.astype(jnp.bfloat16)
    up_call, down_back_call = feed_calls(total, width, up_bias.size)
    act_low, slope = up_call(hidden_low, up_weight, up_bias.reshape(1, -1))
    output, normed_two, factor_two = normalize(
        hidden + project(act_low, down_weight) + vectors[3], vectors[6], vectors[7]
    )
    out_long = output[:split].reshape(rows_here, row_len, width)
    out_short = output[split:].reshape(short_rows, short_len, width)
    upstream = jnp.concatenate(
        [grad_long.reshape(split, width), grad_short.reshape(-1, width)], 0
    ).astype(jnp.float32)
    second_grad, gain_two, shift_two = normalize_back(upstream, normed_two, factor_two, vectors[6])
    down_in = second_grad.astype(jnp.bfloat16)
    down_grad = outer_sum(act_low, down_in)
    down_sum = lax.psum(down_grad.astype(jnp.bfloat16), ("dp", "seq"))
    down_total = jnp.sum(down_in.astype(jnp.float32), 0)
    pre_grad, bias_total = down_back_call(down_in, down_weight, slope)
    up_grad = outer_sum(hidden_low, pre_grad)
    hidden_grad = second_grad + against(pre_grad, up_weight)
    first_grad, gain_one, shift_one = normalize_back(
        hidden_grad, normed_one, factor_one, vectors[4]
    )
    branch_in = first_grad.astype(jnp.bfloat16)
    out_grad = outer_sum(mixture, branch_in)
    out_total = jnp.sum(branch_in.astype(jnp.float32), 0)
    mixture_grad = against(branch_in, out_weight).astype(jnp.bfloat16)
    query_in, key_in, value_in = backward(
        queries, key_rows, value_rows, mixture_grad, seg_column, seg_rows
    )
    query_grad = outer_sum(tokens, query_in)
    key_grad = outer_sum(tokens, key_in)
    value_grad = outer_sum(tokens, value_in)
    token_grad = (
        first_grad
        + against(query_in, query_weight)
        + against(key_in, key_weight)
        + against(value_in, value_weight)
    )
    back_short = token_grad[split:].reshape(short_rows, short_len, width)
    counts = tally(pred_long, target_long, seg_local) + tally(pred_short, target_short, seg_short)
    small = jnp.concatenate(
        [
            jnp.stack(
                [
                    jnp.sum(query_in.astype(jnp.float32), 0),
                    jnp.sum(value_in.astype(jnp.float32), 0),
                    out_total,
                    down_total,
                    gain_one,
                    shift_one,
                    gain_two,
                    shift_two,
                ]
            ),
            bias_total.reshape(-1, width),
            jnp.pad(counts.reshape(1, -1), ((0, 3), (0, width - counts.size))),
        ],
        0,
    )
    squares = [part.astype(jnp.bfloat16) for part in (query_grad, key_grad, value_grad, out_grad)]
    summed, small, returned = reduce_call(
        axes,
        up_grad.astype(jnp.bfloat16),
        squares,
        small,
        token_grad[:split].astype(jnp.bfloat16),
        groups,
    )
    back_long = returned.astype(jnp.float32)
    summed = summed.reshape(-1, width)
    square_start = up_grad.shape[1]
    up_total = jnp.concatenate(
        [summed[i : i + width].astype(jnp.float32) for i in range(0, square_start, width)], 1
    )
    vector_rows = 8 + up_bias.size // width
    return (
        out_long,
        out_short,
        back_long,
        back_short,
        *(
            summed[square_start + i : square_start + i + width].astype(jnp.float32)
            for i in range(0, 4 * width, width)
        ),
        up_total,
        down_sum.astype(jnp.float32),
        small[:8],
        small[8:vector_rows].reshape(-1),
        small[vector_rows, : counts.size].reshape(counts.shape).astype(jnp.int32),
    )


def solution(mesh):
    placed = (
        P("dp", "seq", None),
        P(("dp", "seq"), None, None),
        P("dp", None),
        P(("dp", "seq"), None),
        P("dp", "seq"),
        P("dp", "seq"),
        P(("dp", "seq"), None),
        P(("dp", "seq"), None),
        P(),
        P(),
        P(),
        P(),
        P(),
        P(),
        P(),
        P(),
        P(("dp", "seq"), None, None),
        P(("dp", "seq"), None, None),
    )
    return jax.shard_map(
        functools.partial(local, physical_axes(mesh)),
        mesh=mesh,
        in_specs=placed,
        out_specs=(
            P(("dp", "seq"), None, None),
            P(("dp", "seq"), None, None),
            P("dp", "seq", None),
            P(("dp", "seq"), None, None),
            P(),
            P(),
            P(),
            P(),
            P(),
            P(),
            P(),
            P(),
            P(),
        ),
        check_vma=False,
    )
```

```python
import functools

import jax
import jax.numpy as jnp
from jax import lax
from jax.experimental import pallas as pl
from jax.experimental.pallas import tpu as pltpu
from jax.sharding import PartitionSpec as P

HEADS = 12
VOCAB = 24
LONG_REACH = 256
CHUNKS = 6

epsilon = 1e-05
blocked = -1e30

TAIL = 0.35
SERIES = (
    0.19746604993055228,
    0.19748153788075967,
    0.18507424716028212,
    0.16421743944194458,
    0.10898740989992088,
    0.15459434424968818,
    -0.10693179193342305,
    0.23918706732681347,
    -0.18270557340639457,
    0.042629254353689805,
)


def project(matrix, weight):
    return jnp.dot(matrix, weight, preferred_element_type=jnp.float32)


def outer_sum(first_op, second_op):
    return lax.dot_general(
        first_op, second_op, (((0,), (0,)), ((), ())), preferred_element_type=jnp.float32
    )


def against(matrix, weight):
    return lax.dot_general(
        matrix, weight, (((1,), (1,)), ((), ())), preferred_element_type=jnp.float32
    )


def normalize(residual, gain_row, shift_row):
    centered = residual - jnp.mean(residual, -1, keepdims=True)
    factor = lax.rsqrt(jnp.mean(centered * centered, -1, keepdims=True) + epsilon)
    normed = centered * factor
    return (normed * gain_row + shift_row, normed, factor)


def normalize_back(upward, normed, factor, gain_row):
    scaled = upward * gain_row
    result = factor * (
        scaled
        - jnp.mean(scaled, -1, keepdims=True)
        - normed * jnp.mean(scaled * normed, -1, keepdims=True)
    )
    return (result, jnp.sum(upward * normed, 0), jnp.sum(upward, 0))


def blocks_of(long_len, short_len, short_rows):
    step = 128
    found = []
    for start in range(0, long_len, step):
        low = max(0, (start - LONG_REACH + 1) // step * step)
        high = min(long_len, -(-(start + step + LONG_REACH - 1) // step) * step)
        found.append((start, step, low, high, 0, 0))
    for row in range(short_rows):
        base = long_len + row * short_len
        found.append((base, short_len, base, base + short_len, base, row + 1))
    return found


def fill_bias(col_ref, row_ref, long_bias, short_bias, long_len, short_len, short_rows):
    col = col_ref[0:long_len, :]
    row = row_ref[0:1, 0:long_len]
    long_bias[...] = jnp.where(col == row, 0.0, blocked)
    for index in range(short_rows):
        base = long_len + index * short_len
        col = col_ref[base : base + short_len, :]
        row = row_ref[1 + index : 2 + index, 0:short_len]
        short_bias[index] = jnp.where(col == row, 0.0, blocked)


def bias_at(long_bias, short_bias, first, first_count, low, high, base, index):
    if index == 0:
        return long_bias[first : first + first_count, low:high]
    return short_bias[index - 1]


def two_heads(block, lanes, scale):
    half = block.shape[1] // 2
    zero = jnp.zeros_like(block)
    if scale != 1.0:
        block = block * scale
    return jnp.concatenate(
        [jnp.where(lanes < half, block, zero), jnp.where(lanes < half, zero, block)], 0
    )


def attend_kernel(sizes, scale, q_ref, k_ref, v_ref, col_ref, row_ref, o_ref, long_bias, short_bias):
    @pl.when(pl.program_id(0) == 0)
    def _():
        fill_bias(col_ref, row_ref, long_bias, short_bias, *sizes)

    def scores_of(first, count, low, high, base, index):
        lanes = lax.broadcasted_iota(jnp.int32, (count, 128), 1)
        pair = two_heads(q_ref[first : first + count, :], lanes, scale)
        return against(pair, k_ref[low:high, :])

    blocks = blocks_of(*sizes)
    ahead = scores_of(*blocks[0])
    for place, (first, count, low, high, base, index) in enumerate(blocks):
        scores = ahead
        if place + 1 < len(blocks):
            ahead = scores_of(*blocks[place + 1])
        lanes = lax.broadcasted_iota(jnp.int32, (count, 128), 1)
        bias = bias_at(long_bias, short_bias, first, count, low, high, base, index)
        scores = scores + jnp.concatenate([bias, bias], 0)
        highest = jnp.max(scores, -1, keepdims=True)
        weights = jnp.exp(scores - highest)
        summed = jnp.sum(weights, -1, keepdims=True)
        mixed = project(weights.astype(jnp.bfloat16), v_ref[low:high, :]) / summed
        o_ref[first : first + count, :] = jnp.where(
            lanes < 64, mixed[:count], mixed[count:]
        ).astype(jnp.bfloat16)


def attend_back_kernel(
    sizes,
    scale,
    q_ref,
    k_ref,
    v_ref,
    g_ref,
    col_ref,
    row_ref,
    dq_ref,
    dk_ref,
    dv_ref,
    long_bias,
    short_bias,
    k_sum,
    v_sum,
):
    @pl.when(pl.program_id(0) == 0)
    def _():
        fill_bias(col_ref, row_ref, long_bias, short_bias, *sizes)

    k_sum[...] = jnp.zeros_like(k_sum)
    v_sum[...] = jnp.zeros_like(v_sum)
    def products_of(first, count, low, high, base, index):
        lanes = lax.broadcasted_iota(jnp.int32, (count, 128), 1)
        pair = two_heads(q_ref[first : first + count, :], lanes, scale)
        upward = two_heads(g_ref[first : first + count, :], lanes, 1.0)
        return pair, upward, against(k_ref[low:high, :], pair), against(v_ref[low:high, :], upward)

    blocks = blocks_of(*sizes)
    ahead = products_of(*blocks[0])
    for place, (first, count, low, high, base, index) in enumerate(blocks):
        pair, upward, scores, weight_grad = ahead
        if place + 1 < len(blocks):
            ahead = products_of(*blocks[place + 1])
        lanes = lax.broadcasted_iota(jnp.int32, (count, 128), 1)
        keys = k_ref[low:high, :]
        if index == 0:
            bias = long_bias[low:high, first : first + count]
        else:
            bias = short_bias[index - 1]
        scores = scores + jnp.concatenate([bias, bias], 1)
        highest = jnp.max(scores, 0, keepdims=True)
        weights = jnp.exp(scores - highest)
        weights = weights * (1.0 / jnp.sum(weights, 0, keepdims=True))
        delta = jnp.sum(weights * weight_grad, 0, keepdims=True)
        score_grad = (weights * (weight_grad - delta)).astype(jnp.bfloat16)
        v_sum[low:high, :] += project(weights.astype(jnp.bfloat16), upward)
        k_sum[low:high, :] += project(score_grad, pair)
        q_part = outer_sum(score_grad, keys) * scale
        dq_ref[first : first + count, :] = jnp.where(lanes < 64, q_part[:count], q_part[count:]).astype(
            jnp.bfloat16
        )
    dk_ref[...] = k_sum[...].astype(jnp.bfloat16)
    dv_ref[...] = v_sum[...].astype(jnp.bfloat16)


def attention_calls(sizes, rows, width, scale):
    long_len, short_len, short_rows = sizes
    pairs = width // 128
    column = pl.BlockSpec((rows, 128), lambda i: (0, i))
    col_spec = pl.BlockSpec((rows, 1), lambda i: (0, 0))
    row_spec = pl.BlockSpec((1 + short_rows, long_len), lambda i: (0, 0))
    shape = jax.ShapeDtypeStruct((rows, width), jnp.bfloat16)
    bias = [
        pltpu.VMEM((long_len, long_len), jnp.float32),
        pltpu.VMEM((short_rows, short_len, short_len), jnp.float32),
    ]
    forward = pl.pallas_call(
        functools.partial(attend_kernel, sizes, scale),
        grid=(pairs,),
        in_specs=[column] * 3 + [col_spec, row_spec],
        out_specs=column,
        out_shape=shape,
        scratch_shapes=bias,
        name="attend",
    )
    backward = pl.pallas_call(
        functools.partial(attend_back_kernel, sizes, scale),
        grid=(pairs,),
        in_specs=[column] * 4 + [col_spec, row_spec],
        out_specs=[column] * 3,
        out_shape=[shape] * 3,
        scratch_shapes=bias + [pltpu.VMEM((rows, 128), jnp.float32)] * 2,
        name="attend_back",
    )
    return forward, backward


def gelu_pair(value):
    size = jnp.abs(value)
    part = 1.0 / (1.0 + size * (TAIL * 0.5**0.5))
    series = SERIES[-1]
    for term in SERIES[-2::-1]:
        series = series * part + term
    bell = jnp.exp(value * value * -0.5)
    tail = (0.5 * part) * series * bell
    share = jnp.where(value < 0.0, tail, 1.0 - tail)
    return value * share, share + value * (bell * 0.3989422804014327)


def up_kernel(strips, h_ref, w_ref, b_ref, act_ref, slope_ref):
    rows = h_ref.shape[0] // strips
    for strip in range(strips):
        span = slice(strip * rows, (strip + 1) * rows)
        value = project(h_ref[span, :], w_ref[...]) + b_ref[...]
        act, slope = gelu_pair(value)
        act_ref[span, :] = act.astype(jnp.bfloat16)
        slope_ref[span, :] = slope.astype(jnp.bfloat16)


def down_back_kernel(strips, g_ref, w_ref, slope_ref, out_ref, sum_ref):
    rows = g_ref.shape[0] // strips
    total = jnp.zeros(sum_ref.shape, jnp.float32)
    for strip in range(strips):
        span = slice(strip * rows, (strip + 1) * rows)
        value = against(g_ref[span, :], w_ref[...]) * slope_ref[span, :].astype(jnp.float32)
        low = value.astype(jnp.bfloat16)
        out_ref[span, :] = low
        total += jnp.sum(low.astype(jnp.float32), 0, keepdims=True)
    sum_ref[...] = total


def feed_calls(rows, width, hidden):
    block, strips = 512, 4
    whole = pl.BlockSpec((rows, width), lambda i: (0, 0))
    column = pl.BlockSpec((rows, block), lambda i: (0, i))
    line = pl.BlockSpec((1, block), lambda i: (0, i))
    shape = jax.ShapeDtypeStruct((rows, hidden), jnp.bfloat16)
    up = pl.pallas_call(
        functools.partial(up_kernel, strips),
        grid=(hidden // block,),
        in_specs=[whole, pl.BlockSpec((width, block), lambda i: (0, i)), line],
        out_specs=[column] * 2,
        out_shape=[shape] * 2,
        name="up",
    )
    down_back = pl.pallas_call(
        functools.partial(down_back_kernel, strips),
        grid=(hidden // block,),
        in_specs=[whole, pl.BlockSpec((block, width), lambda i: (i, 0)), column],
        out_specs=[column, line],
        out_shape=[shape, jax.ShapeDtypeStruct((1, hidden), jnp.float32)],
        name="down_back",
    )
    return up, down_back


def physical_axes(mesh):
    first = mesh.devices[0, 0]
    found = {}
    for place, name in enumerate(("x", "y", "z", "core")):

        def at(device):
            return device.core_on_chip if name == "core" else device.coords[place]

        for axis, line in (("dp", mesh.devices[:, 0]), ("seq", mesh.devices[0, :])):
            values = [at(device) - at(first) for device in line]
            size = max(values) + 1
            if size > 1:
                stride = values.index(1)
                assert values == [i // stride % size for i in range(len(values))]
                found[name] = (axis, stride, size)
    return found


def reduce_kernel(axes, orders, chunks, up_ref, down_ref, q_ref, k_ref, v_ref, o_ref, small_ref, token_ref, full, small_out, back, buf, *scratch):
    colors, rows, width = buf.shape
    depth = len(orders[0])
    lands = scratch[:depth]
    small_land, load_sem, send_sem, recv_sem, small_send, small_recv, back_send, back_recv = scratch[depth:]
    chunk = rows // chunks
    spots = {
        name: lax.rem(lax.axis_index(axis) // stride, size)
        for name, (axis, stride, size) in axes.items()
    }

    def peer(name, change):
        axis, stride, size = axes[name]
        target = {other: lax.axis_index(other) for other in ("dp", "seq")}
        target[axis] = target[axis] + change * stride
        return (target["dp"], target["seq"])

    sources = [(up_ref.at[:, i : i + width], 0, i) for i in range(0, up_ref.shape[1], width)]
    sources.append((down_ref, 1, 0))
    sources += [(square, 2, i * width) for i, square in enumerate((q_ref, k_ref, v_ref, o_ref))]
    copies = []
    for source, color, base in sources:
        first, end = base, base + source.shape[0]
        while first < end:
            stop = min(end, (first // chunk + 1) * chunk)
            copies.append(
                (
                    first // chunk,
                    source.at[first - base : stop - base],
                    buf.at[color, first:stop],
                )
            )
            first = stop
    copies.sort(key=lambda item: item[0])
    copies = [
        (k, pltpu.make_async_copy(source, target, load_sem.at[i]))
        for i, (k, source, target) in enumerate(copies)
    ]
    for _, copy in copies:
        copy.start()

    barrier = pltpu.get_barrier_semaphore()
    greeted = 0
    for name, (axis, stride, size) in axes.items():
        for step in range(1, size):
            change = lax.rem(spots[name] + step, size) - spots[name]
            pl.semaphore_signal(
                barrier, inc=1, device_id=peer(name, change), device_id_type=pl.DeviceIdType.MESH
            )
            greeted += 1
    groups, piece = back.shape[:2]
    here, group = lax.axis_index("seq"), lax.axis_index("dp")
    for step in range(1, groups):
        other = lax.rem(here + step, groups)
        pl.semaphore_signal(
            barrier, inc=1, device_id=(group, other), device_id_type=pl.DeviceIdType.MESH
        )
        greeted += 1
    pl.semaphore_wait(barrier, greeted)
    returns = []
    for step in range(1, groups):
        other = lax.rem(here + step, groups)
        returns.append(
            pltpu.make_async_remote_copy(
                src_ref=token_ref.at[pl.ds(pl.multiple_of(other * piece, 16), piece)],
                dst_ref=back.at[here],
                send_sem=back_send.at[step],
                recv_sem=back_recv.at[step],
                device_id=(group, other),
                device_id_type=pl.DeviceIdType.MESH,
            )
        )
        returns[-1].start()
    back[here] = token_ref[pl.ds(pl.multiple_of(here * piece, 16), piece), :]

    def message(color, level, phase, way, k, name, source, target, change):
        return pltpu.make_async_remote_copy(
            src_ref=source,
            dst_ref=target,
            send_sem=send_sem.at[color, level, phase, way, k],
            recv_sem=recv_sem.at[color, level, phase, way, k],
            device_id=peer(name, change),
            device_id_type=pl.DeviceIdType.MESH,
        )

    def plan(color, level, k):
        size = chunk >> (level + 1)
        start = k * chunk
        active = None
        for other in range(level):
            name = orders[color][other]
            last = axes[name][2] - 1
            start = start + jnp.where(spots[name] == last, chunk >> (other + 1), 0)
            if last > 1:
                ends = (spots[name] == 0) | (spots[name] == last)
                active = ends if active is None else active & ends
        return size, start, active

    def guarded(condition, active, body):
        pl.when(condition if active is None else condition & active)(body)

    def reduce_slot(color, level, slot, k):
        name = orders[color][level]
        last = axes[name][2] - 1
        size, start, active = plan(color, level, k)
        for way in range(2):
            place = slot if way == 1 else last - slot
            held = buf.at[color, pl.ds(pl.multiple_of(start + way * size, 16), size)]
            spot = k if lands[level].shape[1] < 2 * chunks * size else 2 * k + way
            land = lands[level].at[color, pl.ds(pl.multiple_of(spot * size, 16), size)]
            change = 1 if way == 1 else -1
            copy = message(color, level, 0, way, k, name, held, land, change)

            into = held
            if level == depth - 1 and slot == last:
                into = full.at[color, pl.ds(pl.multiple_of(start + way * size, 16), size)]

            def body(copy=copy, held=held, land=land, into=into):
                if slot > 0:
                    copy.wait_recv()
                    into[...] = (held[...].astype(jnp.float32) + land[...].astype(jnp.float32)).astype(
                        jnp.bfloat16
                    )
                if slot < last:
                    copy.start()

            guarded(spots[name] == place, active, body)

    def spread_slot(color, level, slot, k):
        name = orders[color][level]
        last = axes[name][2] - 1
        size, start, active = plan(color, level, k)
        for way in range(2):
            place = last - slot if way == 1 else slot
            held = full.at[color, pl.ds(pl.multiple_of(start + way * size, 16), size)]
            change = -1 if way == 1 else 1
            copy = message(color, level, 1, way, k, name, held, held, change)

            def body(copy=copy):
                if slot > 0:
                    copy.wait_recv()
                if slot < last:
                    copy.start()

            guarded(spots[name] == place, active, body)

    def sent(color, level, k):
        name = orders[color][level]
        last = axes[name][2] - 1
        size, start, active = plan(color, level, k)
        for way in range(2):
            held = buf.at[color, pl.ds(pl.multiple_of(start + way * size, 16), size)]
            for phase in range(2):
                copy = message(color, level, phase, way, k, name, held, held, 1)
                stays = spots[name] == (last if (way == 1) == (phase == 0) else 0)
                guarded(jnp.logical_not(stays), active, copy.wait_send)

    small_order = tuple(axes)

    def small_copy(level, step):
        name = small_order[level]
        size = axes[name][2]
        change = lax.rem(spots[name] + step, size) - spots[name]
        slot = sum(axes[other][2] for other in small_order[:level])
        return pltpu.make_async_remote_copy(
            src_ref=small_out,
            dst_ref=small_land.at[slot + step],
            send_sem=small_send.at[slot + step],
            recv_sem=small_recv.at[slot + step],
            device_id=peer(name, change),
            device_id_type=pl.DeviceIdType.MESH,
        )

    def small_start(level):
        for step in range(1, axes[small_order[level]][2]):
            small_copy(level, step).start()

    def small_finish(level):
        name = small_order[level]
        size = axes[name][2]
        slot = sum(axes[other][2] for other in small_order[:level])
        for step in range(1, size):
            small_copy(level, step).wait()
        small_land[slot] = small_out[...]
        total = None
        for place in range(size):
            term = small_land[slot + lax.rem(spots[name] - place + size, size)]
            total = term if total is None else total + term
        small_out[...] = total

    small_out[...] = small_ref[...]
    hops = sum(size - 1 for _, _, size in axes.values())

    work = []
    for color in range(colors):
        base = 0
        for spread in (False, True):
            for level in reversed(range(depth)) if spread else range(depth):
                last = axes[orders[color][level]][2] - 1
                for slot in range(last + 1):
                    work.append((abs(base + slot - hops), base + slot, color, spread, level, slot))
                base += last
    work.sort(key=lambda item: item[:3])

    def tick(t, carry):
        for step in range(chunks):

            @pl.when(t == step)
            def _(step=step):
                for k, copy in copies:
                    if k == step:
                        copy.wait()

        for _, offset, color, spread, level, slot in work:
            k = t - offset

            @pl.when((k >= 0) & (k < chunks))
            def _(color=color, spread=spread, level=level, slot=slot, k=k):
                (spread_slot if spread else reduce_slot)(color, level, slot, k)

        for level in range(depth):

            @pl.when(t == 2 * level)
            def _(level=level):
                small_start(level)

            @pl.when(t == 2 * level + 1)
            def _(level=level):
                small_finish(level)

        return carry

    lax.fori_loop(0, chunks + 2 * hops, tick, 0)

    def drain(k, carry):
        for color in range(colors):
            for level in range(depth):
                sent(color, level, k)
        return carry

    lax.fori_loop(0, chunks, drain, 0)
    for copy in returns:
        copy.wait()


def reduce_call(axes, up, down, squares, small, token, groups):
    rows, width = down.shape
    colors, chunks = 3, CHUNKS
    turn = [name for name in ("x", "y", "z") if name in axes]
    first = [name for name in ("core",) if name in axes]
    orders = [first + turn[i:] + turn[:i] for i in range(3)]
    depth = len(orders[0])
    steps = sum(size for _, _, size in axes.values())
    count = 2 * (up.shape[1] // width + 4 + chunks)
    sems = (colors, depth, 2, 2, chunks)
    lands = [
        rows >> (level + all(axes[order[level]][2] == 2 for order in orders)) for level in range(depth)
    ]
    return pl.pallas_call(
        functools.partial(reduce_kernel, axes, orders, chunks),
        in_specs=[pl.BlockSpec(memory_space=pl.ANY)] * 6 + [pl.BlockSpec(memory_space=pltpu.VMEM)] * 2,
        out_specs=[pl.BlockSpec(memory_space=pltpu.VMEM)] * 3,
        out_shape=[
            jax.ShapeDtypeStruct((colors, rows, width), jnp.bfloat16),
            jax.ShapeDtypeStruct(small.shape, jnp.float32),
            jax.ShapeDtypeStruct((groups, token.shape[0] // groups, width), jnp.bfloat16),
        ],
        scratch_shapes=[pltpu.VMEM((colors, rows, width), jnp.bfloat16)]
        + [pltpu.VMEM((colors, size, width), jnp.bfloat16) for size in lands]
        + [
            pltpu.VMEM((steps,) + small.shape, jnp.float32),
            pltpu.SemaphoreType.DMA((count,)),
            pltpu.SemaphoreType.DMA(sems),
            pltpu.SemaphoreType.DMA(sems),
            pltpu.SemaphoreType.DMA((steps,)),
            pltpu.SemaphoreType.DMA((steps,)),
            pltpu.SemaphoreType.DMA((groups,)),
            pltpu.SemaphoreType.DMA((groups,)),
        ],
        compiler_params=pltpu.CompilerParams(
            collective_id=0, has_side_effects=True, vmem_limit_bytes=60 * 1024 * 1024
        ),
        name="reduce",
    )(up, down, *squares, small, token)


def tally(predicted, target, segment):
    residues = jnp.arange(VOCAB, dtype=jnp.int32)[None, :]
    live_mask = (segment > 0).reshape(-1, 1)
    predicted = predicted.reshape(-1, 1)
    target = target.reshape(-1, 1)
    predicted_hot = (predicted == residues) & live_mask
    target_hot = (target == residues) & live_mask
    hit_hot = target_hot & (predicted == target)
    return jnp.stack(
        [
            jnp.sum(predicted_hot.astype(jnp.float32), 0),
            jnp.sum(target_hot.astype(jnp.float32), 0),
            jnp.sum(hit_hot.astype(jnp.float32), 0),
        ]
    )


def local(
    axes,
    x_long,
    x_short,
    seg_long,
    seg_short,
    pred_long,
    target_long,
    pred_short,
    target_short,
    query_weight,
    key_weight,
    value_weight,
    out_weight,
    up_weight,
    down_weight,
    vectors,
    up_bias,
    grad_long,
    grad_short,
):
    local_len, width = x_long.shape[1:]
    short_rows, short_len = x_short.shape[:2]
    groups = lax.axis_size("seq")
    position = lax.axis_index("seq")
    row_len = local_len * groups
    rows_here = x_long.shape[0] // groups
    split = rows_here * row_len
    total = split + short_rows * short_len
    sizes = (row_len, short_len, short_rows)
    forward, backward = attention_calls(sizes, total, width, (width // HEADS) ** (-0.5))

    seg_row = lax.dynamic_slice_in_dim(seg_long, position * rows_here, rows_here, 0)
    seg_local = lax.dynamic_slice_in_dim(seg_long, position * local_len, local_len, 1)
    seg_rows = jnp.concatenate(
        [seg_row, jnp.pad(seg_short, ((0, 0), (0, row_len - short_len)), constant_values=-1)], 0
    )
    seg_column = jnp.concatenate([seg_row.reshape(-1, 1), seg_short.reshape(-1, 1)], 0)

    moved = lax.all_to_all(x_long, "seq", split_axis=0, concat_axis=1, tiled=True)
    tokens = jnp.concatenate([moved.reshape(split, width), x_short.reshape(-1, width)], 0)
    queries = (project(tokens, query_weight) + vectors[0]).astype(jnp.bfloat16)
    key_rows = project(tokens, key_weight).astype(jnp.bfloat16)
    value_rows = (project(tokens, value_weight) + vectors[1]).astype(jnp.bfloat16)
    mixture = forward(queries, key_rows, value_rows, seg_column, seg_rows)
    branch = project(mixture, out_weight) + vectors[2]
    hidden, normed_one, factor_one = normalize(
        tokens.astype(jnp.float32) + branch, vectors[4], vectors[5]
    )
    hidden_low = hidden.astype(jnp.bfloat16)
    up_call, down_back_call = feed_calls(total, width, up_bias.size)
    act_low, slope = up_call(hidden_low, up_weight, up_bias.reshape(1, -1))
    output, normed_two, factor_two = normalize(
        hidden + project(act_low, down_weight) + vectors[3], vectors[6], vectors[7]
    )
    out_long = output[:split].reshape(rows_here, row_len, width)
    out_short = output[split:].reshape(short_rows, short_len, width)
    upstream = jnp.concatenate(
        [grad_long.reshape(split, width), grad_short.reshape(-1, width)], 0
    ).astype(jnp.float32)
    second_grad, gain_two, shift_two = normalize_back(upstream, normed_two, factor_two, vectors[6])
    down_in = second_grad.astype(jnp.bfloat16)
    down_grad = outer_sum(act_low, down_in)
    down_total = jnp.sum(down_in.astype(jnp.float32), 0)
    pre_grad, bias_total = down_back_call(down_in, down_weight, slope)
    up_grad = outer_sum(hidden_low, pre_grad)
    hidden_grad = second_grad + against(pre_grad, up_weight)
    first_grad, gain_one, shift_one = normalize_back(
        hidden_grad, normed_one, factor_one, vectors[4]
    )
    branch_in = first_grad.astype(jnp.bfloat16)
    out_grad = outer_sum(mixture, branch_in)
    out_total = jnp.sum(branch_in.astype(jnp.float32), 0)
    mixture_grad = against(branch_in, out_weight).astype(jnp.bfloat16)
    query_in, key_in, value_in = backward(
        queries, key_rows, value_rows, mixture_grad, seg_column, seg_rows
    )
    query_grad = outer_sum(tokens, query_in)
    key_grad = outer_sum(tokens, key_in)
    value_grad = outer_sum(tokens, value_in)
    token_grad = (
        first_grad
        + against(query_in, query_weight)
        + against(key_in, key_weight)
        + against(value_in, value_weight)
    )
    back_short = token_grad[split:].reshape(short_rows, short_len, width)
    counts = tally(pred_long, target_long, seg_local) + tally(pred_short, target_short, seg_short)
    small = jnp.concatenate(
        [
            jnp.stack(
                [
                    jnp.sum(query_in.astype(jnp.float32), 0),
                    jnp.sum(value_in.astype(jnp.float32), 0),
                    out_total,
                    down_total,
                    gain_one,
                    shift_one,
                    gain_two,
                    shift_two,
                ]
            ),
            bias_total.reshape(-1, width),
            jnp.pad(counts.reshape(1, -1), ((0, 3), (0, width - counts.size))),
        ],
        0,
    )
    squares = [part.astype(jnp.bfloat16) for part in (query_grad, key_grad, value_grad, out_grad)]
    summed, small, returned = reduce_call(
        axes,
        up_grad.astype(jnp.bfloat16),
        down_grad.astype(jnp.bfloat16),
        squares,
        small,
        token_grad[:split].astype(jnp.bfloat16),
        groups,
    )
    back_long = returned.astype(jnp.float32)
    up_total = jnp.concatenate(
        [summed[0, i : i + width].astype(jnp.float32) for i in range(0, up_grad.shape[1], width)], 1
    )
    vector_rows = 8 + up_bias.size // width
    return (
        out_long,
        out_short,
        back_long,
        back_short,
        *(summed[2, i * width : (i + 1) * width].astype(jnp.float32) for i in range(4)),
        up_total,
        summed[1].astype(jnp.float32),
        small[:8],
        small[8:vector_rows].reshape(-1),
        small[vector_rows, : counts.size].reshape(counts.shape).astype(jnp.int32),
    )


def solution(mesh):
    placed = (
        P("dp", "seq", None),
        P(("dp", "seq"), None, None),
        P("dp", None),
        P(("dp", "seq"), None),
        P("dp", "seq"),
        P("dp", "seq"),
        P(("dp", "seq"), None),
        P(("dp", "seq"), None),
        P(),
        P(),
        P(),
        P(),
        P(),
        P(),
        P(),
        P(),
        P(("dp", "seq"), None, None),
        P(("dp", "seq"), None, None),
    )
    return jax.shard_map(
        functools.partial(local, physical_axes(mesh)),
        mesh=mesh,
        in_specs=placed,
        out_specs=(
            P(("dp", "seq"), None, None),
            P(("dp", "seq"), None, None),
            P("dp", "seq", None),
            P(("dp", "seq"), None, None),
            P(),
            P(),
            P(),
            P(),
            P(),
            P(),
            P(),
            P(),
            P(),
        ),
        check_vma=False,
    )
```

```python
import functools

import jax
import jax.numpy as jnp
from jax import lax
from jax.experimental import pallas as pl
from jax.experimental.pallas import tpu as pltpu
from jax.sharding import PartitionSpec as P

HEADS = 12
VOCAB = 24
LONG_REACH = 256
CHUNKS = 6

epsilon = 1e-05
blocked = -1e30

TAIL = 0.35
SERIES = (
    0.19746604993055228,
    0.19748153788075967,
    0.18507424716028212,
    0.16421743944194458,
    0.10898740989992088,
    0.15459434424968818,
    -0.10693179193342305,
    0.23918706732681347,
    -0.18270557340639457,
    0.042629254353689805,
)


def project(matrix, weight):
    return jnp.dot(matrix, weight, preferred_element_type=jnp.float32)


def outer_sum(first_op, second_op):
    return lax.dot_general(
        first_op, second_op, (((0,), (0,)), ((), ())), preferred_element_type=jnp.float32
    )


def against(matrix, weight):
    return lax.dot_general(
        matrix, weight, (((1,), (1,)), ((), ())), preferred_element_type=jnp.float32
    )


def normalize(residual, gain_row, shift_row):
    centered = residual - jnp.mean(residual, -1, keepdims=True)
    factor = lax.rsqrt(jnp.mean(centered * centered, -1, keepdims=True) + epsilon)
    normed = centered * factor
    return (normed * gain_row + shift_row, normed, factor)


def normalize_back(upward, normed, factor, gain_row):
    scaled = upward * gain_row
    result = factor * (
        scaled
        - jnp.mean(scaled, -1, keepdims=True)
        - normed * jnp.mean(scaled * normed, -1, keepdims=True)
    )
    return (result, jnp.sum(upward * normed, 0), jnp.sum(upward, 0))


def blocks_of(long_len, short_len, short_rows):
    step = 128
    found = []
    for start in range(0, long_len, step):
        low = max(0, (start - LONG_REACH + 1) // step * step)
        high = min(long_len, -(-(start + step + LONG_REACH - 1) // step) * step)
        found.append((start, step, low, high, 0, 0))
    for row in range(short_rows):
        base = long_len + row * short_len
        found.append((base, short_len, base, base + short_len, base, row + 1))
    return found


def fill_bias(col_ref, row_ref, long_bias, short_bias, long_len, short_len, short_rows):
    col = col_ref[0:long_len, :]
    row = row_ref[0:1, 0:long_len]
    long_bias[...] = jnp.where(col == row, 0.0, blocked)
    for index in range(short_rows):
        base = long_len + index * short_len
        col = col_ref[base : base + short_len, :]
        row = row_ref[1 + index : 2 + index, 0:short_len]
        short_bias[index] = jnp.where(col == row, 0.0, blocked)


def bias_at(long_bias, short_bias, first, first_count, low, high, base, index):
    if index == 0:
        return long_bias[first : first + first_count, low:high]
    return short_bias[index - 1]


def two_heads(block, lanes, scale):
    half = block.shape[1] // 2
    zero = jnp.zeros_like(block)
    if scale != 1.0:
        block = block * scale
    return jnp.concatenate(
        [jnp.where(lanes < half, block, zero), jnp.where(lanes < half, zero, block)], 0
    )


def attend_kernel(sizes, scale, q_ref, k_ref, v_ref, col_ref, row_ref, o_ref, long_bias, short_bias):
    @pl.when(pl.program_id(0) == 0)
    def _():
        fill_bias(col_ref, row_ref, long_bias, short_bias, *sizes)

    for first, count, low, high, base, index in blocks_of(*sizes):
        lanes = lax.broadcasted_iota(jnp.int32, (count, 128), 1)
        pair = two_heads(q_ref[first : first + count, :], lanes, scale)
        scores = against(pair, k_ref[low:high, :])
        bias = bias_at(long_bias, short_bias, first, count, low, high, base, index)
        scores = scores + jnp.concatenate([bias, bias], 0)
        highest = jnp.max(scores, -1, keepdims=True)
        weights = jnp.exp(scores - highest)
        summed = jnp.sum(weights, -1, keepdims=True)
        mixed = project(weights.astype(jnp.bfloat16), v_ref[low:high, :]) / summed
        o_ref[first : first + count, :] = jnp.where(
            lanes < 64, mixed[:count], mixed[count:]
        ).astype(jnp.bfloat16)


def attend_back_kernel(
    sizes,
    scale,
    q_ref,
    k_ref,
    v_ref,
    g_ref,
    col_ref,
    row_ref,
    dq_ref,
    dk_ref,
    dv_ref,
    long_bias,
    short_bias,
    k_sum,
    v_sum,
):
    @pl.when(pl.program_id(0) == 0)
    def _():
        fill_bias(col_ref, row_ref, long_bias, short_bias, *sizes)

    k_sum[...] = jnp.zeros_like(k_sum)
    v_sum[...] = jnp.zeros_like(v_sum)
    for first, count, low, high, base, index in blocks_of(*sizes):
        lanes = lax.broadcasted_iota(jnp.int32, (count, 128), 1)
        pair = two_heads(q_ref[first : first + count, :], lanes, scale)
        upward = two_heads(g_ref[first : first + count, :], lanes, 1.0)
        keys = k_ref[low:high, :]
        scores = against(keys, pair)
        if index == 0:
            bias = long_bias[low:high, first : first + count]
        else:
            bias = short_bias[index - 1]
        scores = scores + jnp.concatenate([bias, bias], 1)
        highest = jnp.max(scores, 0, keepdims=True)
        weights = jnp.exp(scores - highest)
        weights = weights * (1.0 / jnp.sum(weights, 0, keepdims=True))
        weight_grad = against(v_ref[low:high, :], upward)
        delta = jnp.sum(weights * weight_grad, 0, keepdims=True)
        score_grad = (weights * (weight_grad - delta)).astype(jnp.bfloat16)
        v_sum[low:high, :] += project(weights.astype(jnp.bfloat16), upward)
        k_sum[low:high, :] += project(score_grad, pair)
        q_part = outer_sum(score_grad, keys) * scale
        dq_ref[first : first + count, :] = jnp.where(lanes < 64, q_part[:count], q_part[count:]).astype(
            jnp.bfloat16
        )
    dk_ref[...] = k_sum[...].astype(jnp.bfloat16)
    dv_ref[...] = v_sum[...].astype(jnp.bfloat16)


def attention_calls(sizes, rows, width, scale):
    long_len, short_len, short_rows = sizes
    pairs = width // 128
    column = pl.BlockSpec((rows, 128), lambda i: (0, i))
    col_spec = pl.BlockSpec((rows, 1), lambda i: (0, 0))
    row_spec = pl.BlockSpec((1 + short_rows, long_len), lambda i: (0, 0))
    shape = jax.ShapeDtypeStruct((rows, width), jnp.bfloat16)
    bias = [
        pltpu.VMEM((long_len, long_len), jnp.float32),
        pltpu.VMEM((short_rows, short_len, short_len), jnp.float32),
    ]
    forward = pl.pallas_call(
        functools.partial(attend_kernel, sizes, scale),
        grid=(pairs,),
        in_specs=[column] * 3 + [col_spec, row_spec],
        out_specs=column,
        out_shape=shape,
        scratch_shapes=bias,
        name="attend",
    )
    backward = pl.pallas_call(
        functools.partial(attend_back_kernel, sizes, scale),
        grid=(pairs,),
        in_specs=[column] * 4 + [col_spec, row_spec],
        out_specs=[column] * 3,
        out_shape=[shape] * 3,
        scratch_shapes=bias + [pltpu.VMEM((rows, 128), jnp.float32)] * 2,
        name="attend_back",
    )
    return forward, backward


def gelu_pair(value):
    size = jnp.abs(value)
    part = 1.0 / (1.0 + size * (TAIL * 0.5**0.5))
    series = SERIES[-1]
    for term in SERIES[-2::-1]:
        series = series * part + term
    bell = jnp.exp(value * value * -0.5)
    tail = (0.5 * part) * series * bell
    share = jnp.where(value < 0.0, tail, 1.0 - tail)
    return value * share, share + value * (bell * 0.3989422804014327)


def up_kernel(strips, h_ref, w_ref, b_ref, act_ref, slope_ref):
    rows = h_ref.shape[0] // strips
    for strip in range(strips):
        span = slice(strip * rows, (strip + 1) * rows)
        value = project(h_ref[span, :], w_ref[...]) + b_ref[...]
        act, slope = gelu_pair(value)
        act_ref[span, :] = act.astype(jnp.bfloat16)
        slope_ref[span, :] = slope.astype(jnp.bfloat16)


def down_back_kernel(strips, g_ref, w_ref, slope_ref, out_ref, sum_ref):
    rows = g_ref.shape[0] // strips
    total = jnp.zeros(sum_ref.shape, jnp.float32)
    for strip in range(strips):
        span = slice(strip * rows, (strip + 1) * rows)
        value = against(g_ref[span, :], w_ref[...]) * slope_ref[span, :].astype(jnp.float32)
        low = value.astype(jnp.bfloat16)
        out_ref[span, :] = low
        total += jnp.sum(low.astype(jnp.float32), 0, keepdims=True)
    sum_ref[...] = total


def feed_calls(rows, width, hidden):
    block, strips = 512, 4
    whole = pl.BlockSpec((rows, width), lambda i: (0, 0))
    column = pl.BlockSpec((rows, block), lambda i: (0, i))
    line = pl.BlockSpec((1, block), lambda i: (0, i))
    shape = jax.ShapeDtypeStruct((rows, hidden), jnp.bfloat16)
    up = pl.pallas_call(
        functools.partial(up_kernel, strips),
        grid=(hidden // block,),
        in_specs=[whole, pl.BlockSpec((width, block), lambda i: (0, i)), line],
        out_specs=[column] * 2,
        out_shape=[shape] * 2,
        name="up",
    )
    down_back = pl.pallas_call(
        functools.partial(down_back_kernel, strips),
        grid=(hidden // block,),
        in_specs=[whole, pl.BlockSpec((block, width), lambda i: (i, 0)), column],
        out_specs=[column, line],
        out_shape=[shape, jax.ShapeDtypeStruct((1, hidden), jnp.float32)],
        name="down_back",
    )
    return up, down_back


def physical_axes(mesh):
    first = mesh.devices[0, 0]
    found = {}
    for place, name in enumerate(("x", "y", "z", "core")):

        def at(device):
            return device.core_on_chip if name == "core" else device.coords[place]

        for axis, line in (("dp", mesh.devices[:, 0]), ("seq", mesh.devices[0, :])):
            values = [at(device) - at(first) for device in line]
            size = max(values) + 1
            if size > 1:
                stride = values.index(1)
                assert values == [i // stride % size for i in range(len(values))]
                found[name] = (axis, stride, size)
    return found


def reduce_kernel(axes, orders, chunks, up_ref, down_ref, q_ref, k_ref, v_ref, o_ref, small_ref, token_ref, full, small_out, back, buf, *scratch):
    colors, rows, width = buf.shape
    depth = len(orders[0])
    lands = scratch[:depth]
    small_land, load_sem, send_sem, recv_sem, small_send, small_recv, back_send, back_recv = scratch[depth:]
    chunk = rows // chunks
    spots = {
        name: lax.rem(lax.axis_index(axis) // stride, size)
        for name, (axis, stride, size) in axes.items()
    }

    def peer(name, change):
        axis, stride, size = axes[name]
        target = {other: lax.axis_index(other) for other in ("dp", "seq")}
        target[axis] = target[axis] + change * stride
        return (target["dp"], target["seq"])

    loads = []
    for block in range(up_ref.shape[1] // width):
        loads.append((up_ref.at[:, block * width : (block + 1) * width], buf.at[0, block * width : (block + 1) * width]))
    loads.append((down_ref, buf.at[1]))
    for block, square in enumerate((q_ref, k_ref, v_ref, o_ref)):
        loads.append((square, buf.at[2, block * width : (block + 1) * width]))
    copies = [
        pltpu.make_async_copy(source, target, load_sem.at[i]) for i, (source, target) in enumerate(loads)
    ]
    for copy in copies:
        copy.start()

    barrier = pltpu.get_barrier_semaphore()
    greeted = 0
    for name, (axis, stride, size) in axes.items():
        for step in range(1, size):
            change = lax.rem(spots[name] + step, size) - spots[name]
            pl.semaphore_signal(
                barrier, inc=1, device_id=peer(name, change), device_id_type=pl.DeviceIdType.MESH
            )
            greeted += 1
    groups, piece = back.shape[:2]
    here, group = lax.axis_index("seq"), lax.axis_index("dp")
    for step in range(1, groups):
        other = lax.rem(here + step, groups)
        pl.semaphore_signal(
            barrier, inc=1, device_id=(group, other), device_id_type=pl.DeviceIdType.MESH
        )
        greeted += 1
    pl.semaphore_wait(barrier, greeted)
    returns = []
    for step in range(1, groups):
        other = lax.rem(here + step, groups)
        returns.append(
            pltpu.make_async_remote_copy(
                src_ref=token_ref.at[pl.ds(pl.multiple_of(other * piece, 16), piece)],
                dst_ref=back.at[here],
                send_sem=back_send.at[step],
                recv_sem=back_recv.at[step],
                device_id=(group, other),
                device_id_type=pl.DeviceIdType.MESH,
            )
        )
        returns[-1].start()
    back[here] = token_ref[pl.ds(pl.multiple_of(here * piece, 16), piece), :]
    for copy in copies:
        copy.wait()

    def message(color, level, phase, way, k, name, source, target, change):
        return pltpu.make_async_remote_copy(
            src_ref=source,
            dst_ref=target,
            send_sem=send_sem.at[color, level, phase, way, k],
            recv_sem=recv_sem.at[color, level, phase, way, k],
            device_id=peer(name, change),
            device_id_type=pl.DeviceIdType.MESH,
        )

    def plan(color, level, k):
        size = chunk >> (level + 1)
        start = k * chunk
        active = None
        for other in range(level):
            name = orders[color][other]
            last = axes[name][2] - 1
            start = start + jnp.where(spots[name] == last, chunk >> (other + 1), 0)
            if last > 1:
                ends = (spots[name] == 0) | (spots[name] == last)
                active = ends if active is None else active & ends
        return size, start, active

    def guarded(condition, active, body):
        pl.when(condition if active is None else condition & active)(body)

    def reduce_slot(color, level, slot, k):
        name = orders[color][level]
        last = axes[name][2] - 1
        size, start, active = plan(color, level, k)
        for way in range(2):
            place = slot if way == 1 else last - slot
            held = buf.at[color, pl.ds(pl.multiple_of(start + way * size, 16), size)]
            spot = k if lands[level].shape[1] < 2 * chunks * size else 2 * k + way
            land = lands[level].at[color, pl.ds(pl.multiple_of(spot * size, 16), size)]
            change = 1 if way == 1 else -1
            copy = message(color, level, 0, way, k, name, held, land, change)

            into = held
            if level == depth - 1 and slot == last:
                into = full.at[color, pl.ds(pl.multiple_of(start + way * size, 16), size)]

            def body(copy=copy, held=held, land=land, into=into):
                if slot > 0:
                    copy.wait_recv()
                    into[...] = (held[...].astype(jnp.float32) + land[...].astype(jnp.float32)).astype(
                        jnp.bfloat16
                    )
                if slot < last:
                    copy.start()

            guarded(spots[name] == place, active, body)

    def spread_slot(color, level, slot, k):
        name = orders[color][level]
        last = axes[name][2] - 1
        size, start, active = plan(color, level, k)
        for way in range(2):
            place = last - slot if way == 1 else slot
            held = full.at[color, pl.ds(pl.multiple_of(start + way * size, 16), size)]
            change = -1 if way == 1 else 1
            copy = message(color, level, 1, way, k, name, held, held, change)

            def body(copy=copy):
                if slot > 0:
                    copy.wait_recv()
                if slot < last:
                    copy.start()

            guarded(spots[name] == place, active, body)

    def sent(color, level, k):
        name = orders[color][level]
        last = axes[name][2] - 1
        size, start, active = plan(color, level, k)
        for way in range(2):
            held = buf.at[color, pl.ds(pl.multiple_of(start + way * size, 16), size)]
            for phase in range(2):
                copy = message(color, level, phase, way, k, name, held, held, 1)
                stays = spots[name] == (last if (way == 1) == (phase == 0) else 0)
                guarded(jnp.logical_not(stays), active, copy.wait_send)

    small_order = tuple(axes)

    def small_copy(level, step):
        name = small_order[level]
        size = axes[name][2]
        change = lax.rem(spots[name] + step, size) - spots[name]
        slot = sum(axes[other][2] for other in small_order[:level])
        return pltpu.make_async_remote_copy(
            src_ref=small_out,
            dst_ref=small_land.at[slot + step],
            send_sem=small_send.at[slot + step],
            recv_sem=small_recv.at[slot + step],
            device_id=peer(name, change),
            device_id_type=pl.DeviceIdType.MESH,
        )

    def small_start(level):
        for step in range(1, axes[small_order[level]][2]):
            small_copy(level, step).start()

    def small_finish(level):
        name = small_order[level]
        size = axes[name][2]
        slot = sum(axes[other][2] for other in small_order[:level])
        for step in range(1, size):
            small_copy(level, step).wait()
        small_land[slot] = small_out[...]
        total = None
        for place in range(size):
            term = small_land[slot + lax.rem(spots[name] - place + size, size)]
            total = term if total is None else total + term
        small_out[...] = total

    small_out[...] = small_ref[...]
    hops = sum(size - 1 for _, _, size in axes.values())

    work = []
    for color in range(colors):
        base = 0
        for spread in (False, True):
            for level in reversed(range(depth)) if spread else range(depth):
                last = axes[orders[color][level]][2] - 1
                for slot in range(last + 1):
                    work.append((abs(base + slot - hops), base + slot, color, spread, level, slot))
                base += last
    work.sort(key=lambda item: item[:3])

    def tick(t, carry):
        for _, offset, color, spread, level, slot in work:
            k = t - offset

            @pl.when((k >= 0) & (k < chunks))
            def _(color=color, spread=spread, level=level, slot=slot, k=k):
                (spread_slot if spread else reduce_slot)(color, level, slot, k)

        for level in range(depth):

            @pl.when(t == 2 * level)
            def _(level=level):
                small_start(level)

            @pl.when(t == 2 * level + 1)
            def _(level=level):
                small_finish(level)

        return carry

    lax.fori_loop(0, chunks + 2 * hops, tick, 0)

    def drain(k, carry):
        for color in range(colors):
            for level in range(depth):
                sent(color, level, k)
        return carry

    lax.fori_loop(0, chunks, drain, 0)
    for copy in returns:
        copy.wait()


def reduce_call(axes, up, down, squares, small, token, groups):
    rows, width = down.shape
    colors, chunks = 3, CHUNKS
    turn = [name for name in ("x", "y", "z") if name in axes]
    first = [name for name in ("core",) if name in axes]
    orders = [first + turn[i:] + turn[:i] for i in range(3)]
    depth = len(orders[0])
    steps = sum(size for _, _, size in axes.values())
    count = up.shape[1] // width + 5
    sems = (colors, depth, 2, 2, chunks)
    lands = [
        rows >> (level + all(axes[order[level]][2] == 2 for order in orders)) for level in range(depth)
    ]
    return pl.pallas_call(
        functools.partial(reduce_kernel, axes, orders, chunks),
        in_specs=[pl.BlockSpec(memory_space=pl.ANY)] * 6 + [pl.BlockSpec(memory_space=pltpu.VMEM)] * 2,
        out_specs=[pl.BlockSpec(memory_space=pltpu.VMEM)] * 3,
        out_shape=[
            jax.ShapeDtypeStruct((colors, rows, width), jnp.bfloat16),
            jax.ShapeDtypeStruct(small.shape, jnp.float32),
            jax.ShapeDtypeStruct((groups, token.shape[0] // groups, width), jnp.bfloat16),
        ],
        scratch_shapes=[pltpu.VMEM((colors, rows, width), jnp.bfloat16)]
        + [pltpu.VMEM((colors, size, width), jnp.bfloat16) for size in lands]
        + [
            pltpu.VMEM((steps,) + small.shape, jnp.float32),
            pltpu.SemaphoreType.DMA((count,)),
            pltpu.SemaphoreType.DMA(sems),
            pltpu.SemaphoreType.DMA(sems),
            pltpu.SemaphoreType.DMA((steps,)),
            pltpu.SemaphoreType.DMA((steps,)),
            pltpu.SemaphoreType.DMA((groups,)),
            pltpu.SemaphoreType.DMA((groups,)),
        ],
        compiler_params=pltpu.CompilerParams(
            collective_id=0, has_side_effects=True, vmem_limit_bytes=60 * 1024 * 1024
        ),
        name="reduce",
    )(up, down, *squares, small, token)


def tally(predicted, target, segment):
    residues = jnp.arange(VOCAB, dtype=jnp.int32)[None, :]
    live_mask = (segment > 0).reshape(-1, 1)
    predicted = predicted.reshape(-1, 1)
    target = target.reshape(-1, 1)
    predicted_hot = (predicted == residues) & live_mask
    target_hot = (target == residues) & live_mask
    hit_hot = target_hot & (predicted == target)
    return jnp.stack(
        [
            jnp.sum(predicted_hot.astype(jnp.float32), 0),
            jnp.sum(target_hot.astype(jnp.float32), 0),
            jnp.sum(hit_hot.astype(jnp.float32), 0),
        ]
    )


def local(
    axes,
    x_long,
    x_short,
    seg_long,
    seg_short,
    pred_long,
    target_long,
    pred_short,
    target_short,
    query_weight,
    key_weight,
    value_weight,
    out_weight,
    up_weight,
    down_weight,
    vectors,
    up_bias,
    grad_long,
    grad_short,
):
    local_len, width = x_long.shape[1:]
    short_rows, short_len = x_short.shape[:2]
    groups = lax.axis_size("seq")
    position = lax.axis_index("seq")
    row_len = local_len * groups
    rows_here = x_long.shape[0] // groups
    split = rows_here * row_len
    total = split + short_rows * short_len
    sizes = (row_len, short_len, short_rows)
    forward, backward = attention_calls(sizes, total, width, (width // HEADS) ** (-0.5))

    seg_row = lax.dynamic_slice_in_dim(seg_long, position * rows_here, rows_here, 0)
    seg_local = lax.dynamic_slice_in_dim(seg_long, position * local_len, local_len, 1)
    seg_rows = jnp.concatenate(
        [seg_row, jnp.pad(seg_short, ((0, 0), (0, row_len - short_len)), constant_values=-1)], 0
    )
    seg_column = jnp.concatenate([seg_row.reshape(-1, 1), seg_short.reshape(-1, 1)], 0)

    moved = lax.all_to_all(x_long, "seq", split_axis=0, concat_axis=1, tiled=True)
    tokens = jnp.concatenate([moved.reshape(split, width), x_short.reshape(-1, width)], 0)
    queries = (project(tokens, query_weight) + vectors[0]).astype(jnp.bfloat16)
    key_rows = project(tokens, key_weight).astype(jnp.bfloat16)
    value_rows = (project(tokens, value_weight) + vectors[1]).astype(jnp.bfloat16)
    mixture = forward(queries, key_rows, value_rows, seg_column, seg_rows)
    branch = project(mixture, out_weight) + vectors[2]
    hidden, normed_one, factor_one = normalize(
        tokens.astype(jnp.float32) + branch, vectors[4], vectors[5]
    )
    hidden_low = hidden.astype(jnp.bfloat16)
    up_call, down_back_call = feed_calls(total, width, up_bias.size)
    act_low, slope = up_call(hidden_low, up_weight, up_bias.reshape(1, -1))
    output, normed_two, factor_two = normalize(
        hidden + project(act_low, down_weight) + vectors[3], vectors[6], vectors[7]
    )
    out_long = output[:split].reshape(rows_here, row_len, width)
    out_short = output[split:].reshape(short_rows, short_len, width)
    upstream = jnp.concatenate(
        [grad_long.reshape(split, width), grad_short.reshape(-1, width)], 0
    ).astype(jnp.float32)
    second_grad, gain_two, shift_two = normalize_back(upstream, normed_two, factor_two, vectors[6])
    down_in = second_grad.astype(jnp.bfloat16)
    down_grad = outer_sum(act_low, down_in)
    down_total = jnp.sum(down_in.astype(jnp.float32), 0)
    pre_grad, bias_total = down_back_call(down_in, down_weight, slope)
    up_grad = outer_sum(hidden_low, pre_grad)
    hidden_grad = second_grad + against(pre_grad, up_weight)
    first_grad, gain_one, shift_one = normalize_back(
        hidden_grad, normed_one, factor_one, vectors[4]
    )
    branch_in = first_grad.astype(jnp.bfloat16)
    out_grad = outer_sum(mixture, branch_in)
    out_total = jnp.sum(branch_in.astype(jnp.float32), 0)
    mixture_grad = against(branch_in, out_weight).astype(jnp.bfloat16)
    query_in, key_in, value_in = backward(
        queries, key_rows, value_rows, mixture_grad, seg_column, seg_rows
    )
    query_grad = outer_sum(tokens, query_in)
    key_grad = outer_sum(tokens, key_in)
    value_grad = outer_sum(tokens, value_in)
    token_grad = (
        first_grad
        + against(query_in, query_weight)
        + against(key_in, key_weight)
        + against(value_in, value_weight)
    )
    back_short = token_grad[split:].reshape(short_rows, short_len, width)
    counts = tally(pred_long, target_long, seg_local) + tally(pred_short, target_short, seg_short)
    small = jnp.concatenate(
        [
            jnp.stack(
                [
                    jnp.sum(query_in.astype(jnp.float32), 0),
                    jnp.sum(value_in.astype(jnp.float32), 0),
                    out_total,
                    down_total,
                    gain_one,
                    shift_one,
                    gain_two,
                    shift_two,
                ]
            ),
            bias_total.reshape(-1, width),
            jnp.pad(counts.reshape(1, -1), ((0, 3), (0, width - counts.size))),
        ],
        0,
    )
    squares = [part.astype(jnp.bfloat16) for part in (query_grad, key_grad, value_grad, out_grad)]
    summed, small, returned = reduce_call(
        axes,
        up_grad.astype(jnp.bfloat16),
        down_grad.astype(jnp.bfloat16),
        squares,
        small,
        token_grad[:split].astype(jnp.bfloat16),
        groups,
    )
    back_long = returned.astype(jnp.float32)
    up_total = summed[0].reshape(-1, width, width).transpose(1, 0, 2).reshape(up_grad.shape)
    up_total = up_total.astype(jnp.float32)
    vector_rows = 8 + up_bias.size // width
    return (
        out_long,
        out_short,
        back_long,
        back_short,
        *(summed[2, i * width : (i + 1) * width].astype(jnp.float32) for i in range(4)),
        up_total,
        summed[1].astype(jnp.float32),
        small[:8],
        small[8:vector_rows].reshape(-1),
        small[vector_rows, : counts.size].reshape(counts.shape).astype(jnp.int32),
    )


def solution(mesh):
    placed = (
        P("dp", "seq", None),
        P(("dp", "seq"), None, None),
        P("dp", None),
        P(("dp", "seq"), None),
        P("dp", "seq"),
        P("dp", "seq"),
        P(("dp", "seq"), None),
        P(("dp", "seq"), None),
        P(),
        P(),
        P(),
        P(),
        P(),
        P(),
        P(),
        P(),
        P(("dp", "seq"), None, None),
        P(("dp", "seq"), None, None),
    )
    return jax.shard_map(
        functools.partial(local, physical_axes(mesh)),
        mesh=mesh,
        in_specs=placed,
        out_specs=(
            P(("dp", "seq"), None, None),
            P(("dp", "seq"), None, None),
            P("dp", "seq", None),
            P(("dp", "seq"), None, None),
            P(),
            P(),
            P(),
            P(),
            P(),
            P(),
            P(),
            P(),
            P(),
        ),
        check_vma=False,
    )
```
